8 devices in a mesh: rep: 2 (over y, z), dp: 4 (over x, core).
Axes of the slice: x: 2, y: 2, z: 1, core: 2. Of those that a mesh axis runs over, the one named last changes fastest.
Arguments:
- x: bfloat16 [8, 2048, 1152], P(('rep', 'dp')), parts along dimension 0
- dy: bfloat16 [8, 2048, 1152], P(('rep', 'dp')), parts along dimension 0
- w_gate: bfloat16 [2, 1152, 4608], P(None, 'dp')
- w_up: bfloat16 [2, 1152, 4608], P(None, 'dp')
- w_down: bfloat16 [2, 4608, 1152], P(None, 'dp')
- m_w_gate: float32 [2, 1152, 4608], P(None, 'dp')
- m_w_up: float32 [2, 1152, 4608], P(None, 'dp')
- m_w_down: float32 [2, 4608, 1152], P(None, 'dp')
- v_w_gate: float32 [2, 1152, 4608], P(None, 'dp')
- v_w_up: float32 [2, 1152, 4608], P(None, 'dp')
- v_w_down: float32 [2, 4608, 1152], P(None, 'dp')
Outputs:
- output 1: bfloat16 [4, 1152, 4608], P('rep', 'dp'), parts along dimension 0
- output 2: bfloat16 [4, 1152, 4608], P('rep', 'dp'), parts along dimension 0
- output 3: bfloat16 [4, 4608, 1152], P('rep', 'dp'), parts along dimension 0
- output 4: float32 [4, 1152, 4608], P('rep', 'dp'), parts along dimension 0
- output 5: float32 [4, 1152, 4608], P('rep', 'dp'), parts along dimension 0
- output 6: float32 [4, 4608, 1152], P('rep', 'dp'), parts along dimension 0
- output 7: float32 [4, 1152, 4608], P('rep', 'dp'), parts along dimension 0
- output 8: float32 [4, 1152, 4608], P('rep', 'dp'), parts along dimension 0
- output 9: float32 [4, 4608, 1152], P('rep', 'dp'), parts along dimension 0
There are 2 independent parts. The reference program is written for one: setup_inputs(seed, part) draws one part's arguments, and reference() takes and returns one part's arrays. A program takes and returns all parts, laid end to end along the dimension named above; an argument that names none is the same for every part.
All inputs are finite; a program needn't handle non-finite values.
Results may differ from the reference program's by a relative error of at most 0.022.
Values are sent between devices in bfloat16 or wider.
A program may use at most 2 GiB of HBM per device.

```python
import jax
import jax.numpy as jnp
from jax import lax

SEQUENCES = 4
TOKENS = 2048
D = 1152
FF = 4608
LAYERS = 2
NAMES = ("w_gate", "w_up", "w_down")
SHAPES = {"w_gate": (LAYERS, D, FF), "w_up": (LAYERS, D, FF), "w_down": (LAYERS, FF, D)}


def bump(key, n, height):
    away = (jnp.arange(n, dtype=jnp.int32) - jax.random.randint(key, (), 0, n, jnp.int32)) % n
    return jnp.where(away < n // 8, height, 1.0)


def together(key, own, strength):
    shared = jax.random.normal(key, own.shape[1:], jnp.float32)
    return (own + strength * shared) * lax.rsqrt(1 + strength * strength)


def setup_inputs(seed: int = 0, part: int = 0) -> dict:
    kx, kdy, ka, kb, kz, kf, kh, kl, *keys = jax.random.split(jax.random.key(seed), 8 + 3 * len(NAMES))
    kx, kdy, ka, kb = (jax.random.fold_in(k, part) for k in (kx, kdy, ka, kb))
    kw, km, kv = (keys[i::3] for i in range(3))
    shape = (SEQUENCES, TOKENS, D)
    much_x, much_dy = jax.random.uniform(kz, (2,), jnp.float32, 0.0, 1.0)
    loud = 2.0 ** jax.random.uniform(jax.random.fold_in(kz, 1), (), jnp.float32, -1.0, 2.0)
    layers = 2.0 ** jax.random.uniform(kl, (LAYERS, 1, 1), jnp.float32, -1.0, 1.0)
    x = together(ka, jax.random.normal(kx, shape, jnp.float32), much_x) * bump(kf, D, 4.0)
    dy = together(kb, jax.random.normal(kdy, shape, jnp.float32), much_dy)
    drawn = {"x": x.astype(jnp.bfloat16), "dy": (loud * dy * (SEQUENCES * TOKENS) ** -0.5).astype(jnp.bfloat16)}
    for key, name in zip(kw, NAMES, strict=True):
        w = jax.random.normal(key, SHAPES[name], jnp.float32) * SHAPES[name][1] ** -0.5
        drawn[name] = (w * {"w_gate": 1.0, "w_up": bump(kh, FF, 4.0), "w_down": layers}[name]).astype(jnp.bfloat16)
    for key, name in zip(km, NAMES, strict=True):
        drawn[f"m_{name}"] = 0.1 * jax.random.normal(key, SHAPES[name], jnp.float32)
    for key, name in zip(kv, NAMES, strict=True):
        drawn[f"v_{name}"] = jax.random.uniform(key, SHAPES[name], jnp.float32, 0.005, 0.015)
    return drawn


def matmul(a, w):
    return jnp.dot(a, w, preferred_element_type=jnp.float32).astype(jnp.bfloat16)


def normed(h):
    wide = h.astype(jnp.float32)
    scale = lax.rsqrt(jnp.mean(wide**2, -1, keepdims=True) + 1e-6)
    return (wide * scale).astype(jnp.bfloat16)


def layer(h, w):
    a = normed(h)
    gate = jnp.dot(a, w["w_gate"], preferred_element_type=jnp.float32)
    up = jnp.dot(a, w["w_up"], preferred_element_type=jnp.float32)
    return h + matmul((jax.nn.silu(gate) * up).astype(jnp.bfloat16), w["w_down"])


def adamw(w, m, v, g):
    m = 0.9 * m + 0.1 * g
    v = 0.95 * v + 0.05 * g * g
    step = m * lax.rsqrt(v + 1e-8) + 0.1 * w
    return (w - 0.02 * step).astype(jnp.bfloat16), m, v


def clipped(gradients, sum_of_squares, count):
    factor = jnp.minimum(1.0, 0.5 * lax.rsqrt(sum_of_squares / count + 1e-30))
    return [g * factor for g in gradients]


def stack(weights, h):
    return lax.scan(lambda h, w: (layer(h, w), None), h, weights)[0]


def reference(x, dy, w_gate, w_up, w_down, m_w_gate, m_w_up, m_w_down, v_w_gate, v_w_up, v_w_down):
    weights = dict(zip(NAMES, (w_gate, w_up, w_down), strict=True))

    def take(so_far, sequence):
        h, by_y = sequence
        _, back = jax.vjp(lambda w: stack(w, h), weights)
        return jax.tree.map(lambda total, term: total + term.astype(jnp.float32), so_far, back(by_y)[0]), None

    none_yet = {name: jnp.zeros(w.shape, jnp.float32) for name, w in weights.items()}
    by_weights, _ = lax.scan(take, none_yet, (x, dy))
    gradients = [by_weights[name].astype(jnp.bfloat16).astype(jnp.float32) for name in NAMES]
    gradients = clipped(gradients, sum(jnp.sum(g * g) for g in gradients), sum(g.size for g in gradients))
    new = [
        adamw(w.astype(jnp.float32), m, v, g)
        for w, m, v, g in zip((w_gate, w_up, w_down), (m_w_gate, m_w_up, m_w_down), (v_w_gate, v_w_up, v_w_down), gradients, strict=True)
    ]
    return tuple(one[which] for which in range(3) for one in new)
```

```python
import jax
import jax.numpy as jnp
from jax import lax
from jax.experimental import pallas as pl
from jax.experimental.pallas import tpu as pltpu
from jax.sharding import PartitionSpec as P

MESH = pl.DeviceIdType.MESH
T, D, FF, L = 2048, 1152, 4608, 2
BG, BD = D // 4, FF // 4
FQ = 1152
F32, BF16 = jnp.float32, jnp.bfloat16
ANY = pl.BlockSpec(memory_space=pl.ANY)


def nn(a, b):
    return lax.dot_general(a, b, (((1,), (0,)), ((), ())), preferred_element_type=F32)


def nt(a, b):
    return lax.dot_general(a, b, (((1,), (1,)), ((), ())), preferred_element_type=F32)


def tn(a, b):
    return lax.dot_general(a, b, (((0,), (0,)), ((), ())), preferred_element_type=F32)


def mega(x, dy, wg, wu, wd, *refs):
    (gg, gu, gd, sqg, sqd, GU, WD, A, AT, H1, HID, PRE, DG, DX, SC, RC, SX, RX, OWN, SCD, RCD, SXD, RXD, OWND, *sems) = refs
    ag_send, ag_recv, c_send, c_recv, x_send, x_recv, load_sem = sems
    r, d = lax.axis_index("rep"), lax.axis_index("dp")
    xx, cc = d // 2, d % 2
    dc, dx_, dxc = 2 * xx + 1 - cc, 2 * (1 - xx) + cc, 2 * (1 - xx) + 1 - cc
    to_c, to_x, to_y = (r, dc), (r, dx_), (1 - r, d)

    barrier = pltpu.get_barrier_semaphore()
    for to in (to_c, to_x, to_y):
        pl.semaphore_signal(barrier, inc=1, device_id=to, device_id_type=MESH)
    pl.semaphore_wait(barrier, 3)

    def remote(src, dst, s, q, to):
        return pltpu.make_async_remote_copy(src_ref=src, dst_ref=dst, send_sem=s, recv_sem=q, device_id=to, device_id_type=MESH)

    units = []
    for layer in range(L):
        for q in range(FF // FQ):
            cols = pl.ds(q * FQ, FQ)
            units.append([(wg, GU.at[layer, 0], layer, BG, 0, BG, cols), (wu, GU.at[layer, 1], layer, BG, 0, BG, cols)])
        for half in range(2):
            units.append([(wd, WD.at[layer], layer, BD, half * (BD // 2), BD // 2, pl.ds(0, D))])

    def flow(u, hop):
        out = []
        for i, (arg, full, layer, block, r0, rows, cols) in enumerate(units[u]):
            half = rows // 2
            mine = pl.ds(r0 + r * half, half)
            s, q = ag_send.at[u, i, hop], ag_recv.at[u, i, hop]
            if hop == 0:
                out.append(remote(arg.at[layer, mine, cols], full.at[pl.ds(d * block + r0 + r * half, half), cols], s, q, to_x))
            elif hop == 1:
                at = full.at[pl.ds(dx_ * block + r0 + r * half, half), cols]
                out.append(remote(at, at, s, q, to_y))
            elif hop == 2:
                out.append(remote(arg.at[layer, pl.ds(r0, rows), cols], full.at[pl.ds(d * block + r0, rows), cols], s, q, to_c))
            else:
                at = full.at[pl.ds(dx_ * block + r0, rows), cols]
                out.append(remote(at, at, s, q, to_c))
        return out

    def start(u, hop):
        for c in flow(u, hop):
            c.start()

    def arrive(u, hop):
        for c in flow(u, hop):
            c.wait_recv()

    n_units = len(units)
    for u in range(n_units):
        start(u, 0)
    for u in range(n_units):
        start(u, 2)

    def to_y_hop(u):
        if u < n_units:
            arrive(u, 0)
            start(u, 1)

    def to_c_hop(u):
        arrive(u, 1)
        start(u, 3)

    def whole(u):
        arrive(u, 2)
        arrive(u, 3)

    def load(dst, arg, full, layer, block, cols, base=0):
        out = [pltpu.make_async_copy(arg.at[layer, :, cols], dst.at[pl.ds(d * block, block), :], load_sem.at[base])]
        for i, b in enumerate((dc, dx_, dxc)):
            out.append(pltpu.make_async_copy(full.at[pl.ds(b * block, block), cols], dst.at[pl.ds(b * block, block), :], load_sem.at[base + 1 + i]))
        return out

    def run(copies):
        for c in copies:
            c.start()
        for c in copies:
            c.wait()

    def norm_of(h):
        wide = h.astype(F32)
        scale = lax.rsqrt(jnp.mean(wide * wide, -1, keepdims=True) + 1e-6)
        return wide * scale

    def norm_body(x_ref, a_ref, at_ref):
        a = norm_of(x_ref[...])
        a_ref[...] = a.astype(BF16)
        at_ref[...] = a.T.astype(BF16)

    def norm():
        b = 512
        pltpu.emit_pipeline(
            norm_body, grid=(T // b,), in_specs=[pl.BlockSpec((b, D), lambda i: (i, 0))],
            out_specs=[pl.BlockSpec((b, D), lambda i: (i, 0)), pl.BlockSpec((D, b), lambda i: (0, i))],
        )(x, A.at[0], AT.at[0])

    def gate_up(layer, q):
        def scoped(w):
            cols = pl.ds(q * FQ, FQ)
            run(load(w.at[0], wg, GU.at[layer, 0], layer, BG, cols) + load(w.at[1], wu, GU.at[layer, 1], layer, BG, cols, 4))

            def body(a_ref, gate_ref, up_ref, hid_ref):
                a = a_ref[...]
                gate, up = nn(a, w[0]), nn(a, w[1])
                gate_ref[...] = gate
                up_ref[...] = up
                hid_ref[...] = (gate * jax.nn.sigmoid(gate) * up).astype(BF16)

            b = 512
            out = pl.BlockSpec((b, FQ), lambda i: (i, q))
            pltpu.emit_pipeline(
                body, grid=(T // b,), in_specs=[pl.BlockSpec((b, D), lambda i: (i, 0))], out_specs=[out, out, out],
            )(A.at[layer], PRE.at[layer, 0], PRE.at[layer, 1], HID.at[layer])

        pl.run_scoped(scoped, pltpu.VMEM((2, D, FQ), BF16))

    def down():
        def scoped(w):
            run(load(w, wd, WD.at[0], 0, BD, pl.ds(0, D)))

            def body(x_ref, hid_ref, h_ref, a_ref, at_ref):
                h = x_ref[...] + nn(hid_ref[...], w[...]).astype(BF16)
                h_ref[...] = h
                a = norm_of(h)
                a_ref[...] = a.astype(BF16)
                at_ref[...] = a.T.astype(BF16)

            b = 256
            row = pl.BlockSpec((b, D), lambda i: (i, 0))
            pltpu.emit_pipeline(
                body, grid=(T // b,), in_specs=[row, pl.BlockSpec((b, FF), lambda i: (i, 0))],
                out_specs=[row, row, pl.BlockSpec((D, b), lambda i: (0, i))],
            )(x, HID.at[0], H1, A.at[1], AT.at[1])

        pl.run_scoped(scoped, pltpu.VMEM((FF, D), BF16))

    def by_hidden(layer):
        by = dy if layer else DX

        def scoped(w):
            run(load(w, wd, WD.at[layer], layer, BD, pl.ds(0, D)))

            def body(by_ref, gate_ref, up_ref, bg_ref, bu_ref):
                j = pl.program_id(1)
                rows = pl.ds(pl.multiple_of(j * FQ, FQ), FQ)
                by_hid = nt(by_ref[...], w[rows, :]).astype(BF16).astype(F32)
                gate, up = gate_ref[...], up_ref[...]
                s = jax.nn.sigmoid(gate)
                silu = gate * s
                bu_ref[...] = (by_hid * silu).astype(BF16)
                bg_ref[...] = (by_hid * up * (s + silu * (1 - s))).astype(BF16)

            b = 512
            tile = pl.BlockSpec((b, FQ), lambda i, j: (i, j))
            pltpu.emit_pipeline(
                body, grid=(T // b, FF // FQ), in_specs=[pl.BlockSpec((b, D), lambda i, j: (i, 0)), tile, tile],
                out_specs=[tile, tile],
            )(by, PRE.at[layer, 0], PRE.at[layer, 1], DG.at[layer, 0], DG.at[layer, 1])

        pl.run_scoped(scoped, pltpu.VMEM((FF, D), BF16))

    def by_input():
        def scoped(wg_, wu_):
            every = pl.ds(0, FF)
            run(load(wg_, wg, GU.at[1, 0], 1, BG, every) + load(wu_, wu, GU.at[1, 1], 1, BG, every, 4))

            def body(bg_ref, bu_ref, h_ref, dy_ref, out_ref):
                by_a = nt(bg_ref[...], wg_[...]).astype(BF16).astype(F32) + nt(bu_ref[...], wu_[...]).astype(BF16).astype(F32)
                by_a = by_a.astype(BF16).astype(F32)
                wide = h_ref[...].astype(F32)
                scale = lax.rsqrt(jnp.mean(wide * wide, -1, keepdims=True) + 1e-6)
                along = jnp.mean(by_a * wide, -1, keepdims=True)
                by_h = by_a * scale - wide * (scale * scale * scale * along)
                out_ref[...] = dy_ref[...] + by_h.astype(BF16)

            b = 256
            row, wide_row = pl.BlockSpec((b, D), lambda i: (i, 0)), pl.BlockSpec((b, FF), lambda i: (i, 0))
            pltpu.emit_pipeline(
                body, grid=(T // b,), in_specs=[wide_row, wide_row, row, row], out_specs=[row],
            )(DG.at[1, 0], DG.at[1, 1], H1, dy, DX)

        pl.run_scoped(scoped, pltpu.VMEM((D, FF), BF16), pltpu.VMEM((D, FF), BF16))

    def send_c(i):
        s, q = (SC, RC) if i < 4 else (SCD, RCD)
        k = i if i < 4 else i - 4
        return remote(s.at[k], q.at[k], c_send.at[i], c_recv.at[i], to_c)

    def send_x(i):
        s, q = (SX, RX) if i < 4 else (SXD, RXD)
        k = i if i < 4 else i - 4
        return remote(s.at[k], q.at[k], x_send.at[i], x_recv.at[i], to_x)

    def grad_gu(layer, m, first):
        i = 2 * layer + m

        def scoped(lhs):
            one, two = (dxc, dc) if first else (dx_, d)
            run([
                pltpu.make_async_copy(AT.at[layer, pl.ds(one * BG, BG), :], lhs.at[pl.ds(0, BG), :], load_sem.at[0]),
                pltpu.make_async_copy(AT.at[layer, pl.ds(two * BG, BG), :], lhs.at[pl.ds(BG, BG), :], load_sem.at[1]),
            ])
            b = 512
            by = pl.BlockSpec((T, b), lambda j: (0, j))
            both = pl.BlockSpec((2, BG, b), lambda j: (0, 0, j))
            single = pl.BlockSpec((BG, b), lambda j: (0, j))
            if first:
                def body(by_ref, out_ref):
                    g = nn(lhs[...], by_ref[...]).astype(BF16)
                    out_ref[0] = g[:BG]
                    out_ref[1] = g[BG:]

                pltpu.emit_pipeline(body, grid=(FF // b,), in_specs=[by], out_specs=[both])(DG.at[layer, m], SC.at[i])
            else:
                def body(by_ref, came_ref, x_ref, own_ref):
                    g = nn(lhs[...], by_ref[...]).astype(BF16).astype(F32)
                    x_ref[...] = (g[:BG] + came_ref[0].astype(F32)).astype(BF16)
                    own_ref[...] = g[BG:] + came_ref[1].astype(F32)

                pltpu.emit_pipeline(body, grid=(FF // b,), in_specs=[by, both], out_specs=[single, single])(
                    DG.at[layer, m], RC.at[i], SX.at[i], OWN.at[i])

        pl.run_scoped(scoped, pltpu.VMEM((2 * BG, T), BF16))

    def grad_d(layer, first):
        by = dy if layer else DX
        core = 1 - cc if first else cc

        def scoped(rhs):
            run([pltpu.make_async_copy(by, rhs, load_sem.at[0])])
            b = 384
            n = BD // b

            def hid_at(k, j):
                block = 2 * ((1 - xx) * (1 - k) + xx * k) + core
                return 0, block * n + j

            hid = pl.BlockSpec((T, b), hid_at)
            out = pl.BlockSpec((1, b, D), lambda k, j: (k, j, 0))
            if first:
                def body(hid_ref, out_ref):
                    out_ref[0] = tn(hid_ref[...], rhs[...]).astype(BF16)

                pltpu.emit_pipeline(body, grid=(2, n), in_specs=[hid], out_specs=[out])(HID.at[layer], SCD.at[layer])
            else:
                def one(k, outs):
                    def body(hid_ref, came_ref, out_ref):
                        g = tn(hid_ref[...], rhs[...]).astype(BF16).astype(F32) + came_ref[...].astype(F32)
                        out_ref[...] = g.astype(out_ref.dtype)

                    row = pl.BlockSpec((b, D), lambda j: (j, 0))
                    pltpu.emit_pipeline(
                        body, grid=(n,), in_specs=[pl.BlockSpec((T, b), lambda j: hid_at(k, j)), row], out_specs=[row],
                    )(HID.at[layer], RCD.at[layer, k], outs)

                one(0, SXD.at[layer])
                send_x(4 + layer).start()
                one(1, OWND.at[layer])

        pl.run_scoped(scoped, pltpu.VMEM((T, D), BF16))

    def finish(i, total, first):
        send_x(i).wait_recv()
        own, came, out = (OWN.at[i], RX.at[i], (gg, gu)[i % 2].at[i // 2]) if i < 4 else (OWND.at[i - 4], RXD.at[i - 4], gd.at[i - 4])
        rows, cols = (BG, FF) if i < 4 else (BD, D)
        b = 96 if i < 4 else 384
        if first:
            total[...] = jnp.zeros_like(total)

        def body(own_ref, came_ref, out_ref):
            g = (own_ref[...] + came_ref[...].astype(F32)).astype(BF16)
            out_ref[...] = g
            g = g.astype(F32)
            total[...] += jnp.sum((g * g).reshape(b // 8, 8, cols), axis=0)

        row = pl.BlockSpec((b, cols), lambda j: (j, 0))
        pltpu.emit_pipeline(body, grid=(rows // b,), in_specs=[row, row], out_specs=[row])(own, came, out)

    norm()
    to_y_hop(0)
    to_y_hop(1)
    step = 0

    def usable(u):
        to_c_hop(u)
        to_y_hop(u + 2)
        whole(u)

    for q in range(4):
        usable(q)
        gate_up(0, q)
    usable(4)
    usable(5)
    down()
    for q in range(4):
        usable(6 + q)
        gate_up(1, q)
    grad_d(1, True)
    send_c(5).start()
    usable(10)
    usable(11)
    send_c(5).wait_recv()
    grad_d(1, False)
    by_hidden(1)
    grad_gu(1, 0, True)
    send_c(2).start()
    grad_gu(1, 1, True)
    send_c(3).start()
    send_c(2).wait_recv()
    grad_gu(1, 0, False)
    send_x(2).start()
    send_c(3).wait_recv()
    grad_gu(1, 1, False)
    send_x(3).start()
    by_input()
    grad_d(0, True)
    send_c(4).start()
    by_hidden(0)
    send_c(4).wait_recv()
    grad_d(0, False)
    grad_gu(0, 0, True)
    send_c(0).start()
    grad_gu(0, 1, True)
    send_c(1).start()
    send_c(0).wait_recv()
    grad_gu(0, 0, False)
    send_x(0).start()
    send_c(1).wait_recv()
    grad_gu(0, 1, False)
    send_x(1).start()
    for n, i in enumerate((5, 4)):
        finish(i, sqd, n == 0)
    for n, i in enumerate((2, 3, 0, 1)):
        finish(i, sqg, n == 0)
    for u in range(n_units):
        for hop in range(4):
            for c in flow(u, hop):
                c.wait_send()
    for i in range(6):
        send_c(i).wait_send()
        send_x(i).wait_send()


def fused(x, dy, wg, wu, wd):
    def hbm(shape, dtype):
        return jax.ShapeDtypeStruct(shape, dtype)

    outs = [
        hbm((L, BG, FF), BF16), hbm((L, BG, FF), BF16), hbm((L, BD, D), BF16), hbm((8, FF), F32), hbm((8, D), F32),
        hbm((L, 2, D, FF), BF16), hbm((L, FF, D), BF16), hbm((L, T, D), BF16), hbm((L, D, T), BF16), hbm((T, D), BF16), hbm((L, T, FF), BF16),
        hbm((L, 2, T, FF), F32), hbm((L, 2, T, FF), BF16), hbm((T, D), BF16),
        hbm((4, 2, BG, FF), BF16), hbm((4, 2, BG, FF), BF16), hbm((4, BG, FF), BF16), hbm((4, BG, FF), BF16), hbm((4, BG, FF), F32),
        hbm((2, 2, BD, D), BF16), hbm((2, 2, BD, D), BF16), hbm((2, BD, D), BF16), hbm((2, BD, D), BF16), hbm((2, BD, D), F32),
    ]
    specs = [ANY] * len(outs)
    specs[3] = specs[4] = pl.BlockSpec(memory_space=pltpu.VMEM)
    dma = pltpu.SemaphoreType.DMA
    return pl.pallas_call(
        mega,
        out_shape=outs,
        in_specs=[ANY] * 5,
        out_specs=specs,
        scratch_shapes=[dma((12, 2, 4)), dma((12, 2, 4)), dma((6,)), dma((6,)), dma((6,)), dma((6,)), dma((8,))],
        compiler_params=pltpu.CompilerParams(collective_id=0, has_side_effects=True, vmem_limit_bytes=60 * 2**20),
        name="step",
    )(x, dy, wg, wu, wd)[:5]


def adamw(w, m, v, g):
    m = 0.9 * m + 0.1 * g
    v = 0.95 * v + 0.05 * g * g
    step = m * lax.rsqrt(v + 1e-8) + 0.1 * w
    return (w - 0.02 * step).astype(BF16), m, v


def solution(mesh):
    def step(x, dy, *arrays):
        weights, m, v = (arrays[i : i + 3] for i in (0, 3, 6))
        *gradients, sqg, sqd = fused(x[0], dy[0], *weights)
        squares = lax.psum(jnp.sum(sqg) + jnp.sum(sqd), "dp")
        count = lax.psum(1, "dp") * sum(g.size for g in gradients)
        factor = jnp.minimum(1.0, 0.5 * lax.rsqrt(squares / count + 1e-30))
        new = [adamw(w.astype(F32), m, v, g.astype(F32) * factor) for w, m, v, g in zip(weights, m, v, gradients, strict=True)]
        return tuple(one[which] for which in range(3) for one in new)

    states, cut = P(("rep", "dp"), None, None), P(None, "dp", None)
    return jax.shard_map(
        step,
        mesh=mesh,
        in_specs=(states, states) + (cut,) * 9,
        out_specs=(P("rep", "dp", None),) * 9,
        check_vma=False,
    )
```

```python
import jax
import jax.numpy as jnp
from jax import lax
from jax.experimental import pallas as pl
from jax.experimental.pallas import tpu as pltpu
from jax.sharding import PartitionSpec as P

MESH = pl.DeviceIdType.MESH
T, D, FF, L = 2048, 1152, 4608, 2
BG, BD = D // 4, FF // 4
FU = 768
NU = FF // FU
F32, BF16 = jnp.float32, jnp.bfloat16
ANY = pl.BlockSpec(memory_space=pl.ANY)


def nn(a, b):
    return lax.dot_general(a, b, (((1,), (0,)), ((), ())), preferred_element_type=F32)


def nt(a, b):
    return lax.dot_general(a, b, (((1,), (1,)), ((), ())), preferred_element_type=F32)


def tn(a, b):
    return lax.dot_general(a, b, (((0,), (0,)), ((), ())), preferred_element_type=F32)


def mega(x, dy, wg, wu, wd, *refs):
    (gg, gu, gd, sq, GU, WD, AT, H1, HID, PRE, DH, DG, SC, RC, SX, RX, OWN, SCD, RCD, SXD, RXD, OWND) = refs[:22]
    (wgu, wdv, a_all, by_all, tot_g, tot_d, sq_all) = refs[22:29]
    (gs, gr, ds_, dr, c_send, c_recv, x_send, x_recv, sq_send, sq_recv, load_sem, wd_sem, by_sem) = refs[29:]
    r, d = lax.axis_index("rep"), lax.axis_index("dp")
    xx, cc = d // 2, d % 2
    dc, dx_, dxc = 2 * xx + 1 - cc, 2 * (1 - xx) + cc, 2 * (1 - xx) + 1 - cc
    to_c, to_x, to_xc, to_y = (r, dc), (r, dx_), (r, dxc), (1 - r, d)

    barrier = pltpu.get_barrier_semaphore()
    for to in (to_c, to_x, to_xc, to_y):
        pl.semaphore_signal(barrier, inc=1, device_id=to, device_id_type=MESH)
    pl.semaphore_wait(barrier, 4)

    def remote(src, dst, s, q, to):
        return pltpu.make_async_remote_copy(src_ref=src, dst_ref=dst, send_sem=s, recv_sem=q, device_id=to, device_id_type=MESH)

    def piece(arg, full, layer, block, r0, rows, cols, s, q, hop):
        half = rows // 2
        if hop == 0:
            mine = r0 + r * half
            return remote(arg.at[layer, pl.ds(mine, half), cols], full.at[pl.ds(d * block + mine, half), cols], s, q, to_x)
        if hop == 1:
            at = full.at[pl.ds(dx_ * block + r0 + r * half, half), cols]
            return remote(at, at, s, q, to_y)
        if hop == 2:
            return remote(arg.at[layer, pl.ds(r0, rows), cols], full.at[pl.ds(d * block + r0, rows), cols], s, q, to_c)
        at = full.at[pl.ds(dx_ * block + r0, rows), cols]
        return remote(at, at, s, q, to_c)

    def columns(u):
        return pl.ds(u * FU if isinstance(u, int) else pl.multiple_of(u * FU, FU), FU)

    class Gate:
        def __init__(self, layer, u):
            self.layer, self.u = layer, u

        def copies(self, hop):
            layer, u = self.layer, self.u
            return [piece(arg, GU.at[layer, m], layer, BG, 0, BG, columns(u), gs.at[layer, u, m, hop], gr.at[layer, u, m, hop], hop)
                    for m, arg in enumerate((wg, wu))]

    class Down:
        def __init__(self, layer, u):
            self.layer, self.u = layer, u

        def copies(self, hop):
            layer, u = self.layer, self.u
            return [piece(wd, WD.at[layer], layer, BD, u * (BD // 2), BD // 2, pl.ds(0, D), ds_.at[layer, u, hop], dr.at[layer, u, hop], hop)]

    def start(unit, hop):
        for c in unit.copies(hop):
            c.start()

    def arrive(unit, hop):
        for c in unit.copies(hop):
            c.wait_recv()

    def on_y(unit):
        arrive(unit, 0)
        start(unit, 1)

    def on_c(unit):
        arrive(unit, 1)
        start(unit, 3)

    def whole(unit):
        arrive(unit, 2)
        arrive(unit, 3)

    every = [Gate(0, u) for u in range(NU)] + [Down(0, 0), Down(0, 1), Down(1, 0), Down(1, 1)] + [Gate(1, u) for u in range(NU)]
    for unit in every:
        start(unit, 0)
    for unit in every:
        start(unit, 2)
    pltpu.make_async_copy(dy, by_all, by_sem).start()

    def gate_loads(layer, u):
        out = []
        for m, arg in enumerate((wg, wu)):
            for i, b in enumerate((d, dc, dx_, dxc)):
                rows = pl.ds(b * BG, BG)
                src = GU.at[layer, m, rows, columns(u)] if i else arg.at[layer, :, columns(u)]
                out.append(pltpu.make_async_copy(src, wgu.at[m, rows, columns(u)], load_sem.at[m, i]))
        return out

    def down_loads(layer):
        out = []
        for i, b in enumerate((d, dc, dx_, dxc)):
            rows = pl.ds(b * BD, BD)
            out.append(pltpu.make_async_copy(WD.at[layer, rows, :] if i else wd.at[layer], wdv.at[rows, :], wd_sem.at[b]))
        return out

    def begin(copies):
        for c in copies:
            c.start()

    def end(copies):
        for c in copies:
            c.wait()

    def down_here(layer, b):
        rows = pl.ds(b * BD, BD)
        pltpu.make_async_copy(WD.at[layer, rows, :], wdv.at[rows, :], wd_sem.at[b]).wait()

    def norm_of(h):
        wide = h.astype(F32)
        scale = lax.rsqrt(jnp.mean(wide * wide, -1, keepdims=True) + 1e-6)
        return wide * scale

    def rows_of(i, b):
        return pl.ds(pl.multiple_of(i * b, b), b)

    def at_steps(step, hooks):
        for when, what in hooks.items():

            @pl.when(step == when)
            def _(what=what):
                what()

    def norm():
        b = 512

        def body(x_ref, at_ref):
            a = norm_of(x_ref[...])
            a_all[rows_of(pl.program_id(0), b), :] = a.astype(BF16)
            at_ref[...] = a.T.astype(BF16)

        pltpu.emit_pipeline(
            body, grid=(T // b,), in_specs=[pl.BlockSpec((b, D), lambda i: (i, 0))], out_specs=[pl.BlockSpec((D, b), lambda i: (0, i))],
        )(x, AT.at[0])

    def gate_up(layer):
        b = 1024

        def body(*tiles):
            u, t = pl.program_id(0), pl.program_id(1)

            @pl.when(t == 0)
            def _():
                if layer == 0:
                    whole(Gate(layer, u))
                    begin(gate_loads(layer, u))
                end(gate_loads(layer, u))

            @pl.when(t == 1)
            def _():
                if layer == 0:
                    pl.when(u + 2 < NU)(lambda: on_y(Gate(0, u + 2)))
                    pl.when(u + 2 == NU)(lambda: on_y(Down(0, 0)))
                    pl.when(u + 1 < NU)(lambda: on_c(Gate(0, u + 1)))
                else:
                    at_steps(u, {0: lambda: (on_y(Gate(1, 5)), on_c(Gate(1, 3))), 1: lambda: on_c(Gate(1, 4)), 2: lambda: on_c(Gate(1, 5))})

                    @pl.when(u + 1 < NU)
                    def _():
                        whole(Gate(layer, u + 1))
                        begin(gate_loads(layer, u + 1))

            a = a_all[rows_of(t, b), :]
            gate, up = nn(a, wgu[0, :, columns(u)]), nn(a, wgu[1, :, columns(u)])
            s = jax.nn.sigmoid(gate)
            silu = gate * s
            if layer == 0:
                gate_ref, up_ref, hid_ref = tiles
                gate_ref[...] = gate
                up_ref[...] = up
            else:
                by_ref, hid_ref, bg_ref, bu_ref = tiles
                by_hid = by_ref[...].astype(F32)
                bu_ref[...] = (by_hid * silu).astype(BF16)
                bg_ref[...] = (by_hid * up * (s + silu * (1 - s))).astype(BF16)
            hid_ref[...] = (silu * up).astype(BF16)

        tile = pl.BlockSpec((b, FU), lambda u, t: (t, u))
        if layer == 0:
            pltpu.emit_pipeline(body, grid=(NU, T // b), in_specs=[], out_specs=[tile] * 3)(PRE.at[0], PRE.at[1], HID.at[0])
        else:
            pltpu.emit_pipeline(body, grid=(NU, T // b), in_specs=[tile], out_specs=[tile] * 3)(DH, HID.at[1], DG.at[1, 0], DG.at[1, 1])

    def down():
        b = 256

        def body(x_ref, hid_ref, h_ref, at_ref):
            i = pl.program_id(0)
            at_steps(i, {
                3: lambda: (on_y(Down(1, 1)), on_c(Down(1, 0))),
                6: lambda: on_y(Gate(1, 0)),
                7: lambda: on_c(Down(1, 1)),
            })
            h = x_ref[...] + nn(hid_ref[...], wdv[...]).astype(BF16)
            h_ref[...] = h
            a = norm_of(h)
            a_all[rows_of(i, b), :] = a.astype(BF16)
            at_ref[...] = a.T.astype(BF16)

        row = pl.BlockSpec((b, D), lambda i: (i, 0))
        pltpu.emit_pipeline(
            body, grid=(T // b,), in_specs=[row, pl.BlockSpec((b, FF), lambda i: (i, 0))],
            out_specs=[row, pl.BlockSpec((D, b), lambda i: (0, i))],
        )(x, HID.at[0], H1, AT.at[1])

    def by_hidden_1():
        b = 1024

        def body(out_ref):
            j, t = pl.program_id(0), pl.program_id(1)
            step = 2 * j + t
            at_steps(step, {
                0: lambda: down_here(1, 0),
                1: lambda: on_y(Gate(1, 1)),
                2: lambda: (down_here(1, 1), on_c(Gate(1, 0))),
                4: lambda: on_y(Gate(1, 2)),
                6: lambda: (down_here(1, 2), on_c(Gate(1, 1))),
                7: lambda: on_y(Gate(1, 3)),
                8: lambda: down_here(1, 3),
                10: lambda: on_c(Gate(1, 2)),
                11: lambda: (on_y(Gate(1, 4)), whole(Gate(1, 0)), begin(gate_loads(1, 0))),
            })
            out_ref[...] = nt(by_all[rows_of(t, b), :], wdv[rows_of(j, FU), :]).astype(BF16)

        pltpu.emit_pipeline(body, grid=(NU, T // b), in_specs=[], out_specs=[pl.BlockSpec((b, FU), lambda j, t: (t, j))])(DH)

    def by_hidden_0():
        b, n = 512, 1152

        def body(gate_ref, up_ref, bg_ref, bu_ref):
            i, j = pl.program_id(0), pl.program_id(1)
            by_hid = nt(by_all[rows_of(i, b), :], wdv[rows_of(j, n), :]).astype(BF16).astype(F32)
            gate, up = gate_ref[...], up_ref[...]
            s = jax.nn.sigmoid(gate)
            silu = gate * s
            bu_ref[...] = (by_hid * silu).astype(BF16)
            bg_ref[...] = (by_hid * up * (s + silu * (1 - s))).astype(BF16)

        deep = pl.BlockSpec((b, n), lambda i, j: (i, j), pipeline_mode=pl.Buffered(3))
        tile = pl.BlockSpec((b, n), lambda i, j: (i, j))
        pltpu.emit_pipeline(body, grid=(T // b, FF // n), in_specs=[deep, deep], out_specs=[tile, tile])(
            PRE.at[0], PRE.at[1], DG.at[0, 0], DG.at[0, 1])

    def by_input():
        b = 256

        def body(bg_ref, bu_ref, h_ref):
            rows = rows_of(pl.program_id(0), b)
            by_a = nt(bg_ref[...], wgu[0]).astype(BF16).astype(F32) + nt(bu_ref[...], wgu[1]).astype(BF16).astype(F32)
            by_a = by_a.astype(BF16).astype(F32)
            wide = h_ref[...].astype(F32)
            scale = lax.rsqrt(jnp.mean(wide * wide, -1, keepdims=True) + 1e-6)
            along = jnp.mean(by_a * wide, -1, keepdims=True)
            by_h = by_a * scale - wide * (scale * scale * scale * along)
            by_all[rows, :] = by_all[rows, :] + by_h.astype(BF16)

        row, wide_row = pl.BlockSpec((b, D), lambda i: (i, 0)), pl.BlockSpec((b, FF), lambda i: (i, 0))
        pltpu.emit_pipeline(body, grid=(T // b,), in_specs=[wide_row, wide_row, row], out_specs=[])(DG.at[1, 0], DG.at[1, 1], H1)

    def send_c(i, k, is_d):
        s, q, e = (SCD, RCD, i + 4) if is_d else (SC, RC, i)
        return remote(s.at[i, k], q.at[i, k], c_send.at[e, k], c_recv.at[e, k], to_c)

    def send_x(i, is_d):
        s, q, e = (SXD, RXD, i + 4) if is_d else (SX, RX, i)
        return remote(s.at[i], q.at[i], x_send.at[e], x_recv.at[e], to_x)

    def grad_gu(layer, m):
        i = 2 * layer + m

        def scoped(lhs):
            b = 768
            by = pl.BlockSpec((T, b), lambda j: (0, j))
            both = pl.BlockSpec((2, BG, b), lambda j: (0, 0, j))
            single = pl.BlockSpec((BG, b), lambda j: (0, j))

            def rows(one, two):
                return [
                    pltpu.make_async_copy(AT.at[layer, pl.ds(one * BG, BG), :], lhs.at[pl.ds(0, BG), :], load_sem.at[0, 0]),
                    pltpu.make_async_copy(AT.at[layer, pl.ds(two * BG, BG), :], lhs.at[pl.ds(BG, BG), :], load_sem.at[0, 1]),
                ]

            first, second = rows(dxc, dc), rows(dx_, d)
            begin(first)

            def body_c(by_ref, out_ref):
                pl.when(pl.program_id(0) == 0)(lambda: end(first))
                g = nn(lhs[...], by_ref[...]).astype(BF16)
                out_ref[0] = g[:BG]
                out_ref[1] = g[BG:]

            pltpu.emit_pipeline(body_c, grid=(FF // b,), in_specs=[by], out_specs=[both])(DG.at[layer, m], SC.at[i])
            begin(second)
            send_c(i, 0, False).start()
            send_c(i, 1, False).start()
            send_c(i, 0, False).wait_recv()

            def body_x(by_ref, came_ref, x_ref, own_ref):
                pl.when(pl.program_id(0) == 0)(lambda: end(second))
                g = nn(lhs[...], by_ref[...]).astype(BF16)
                x_ref[...] = (g[:BG].astype(F32) + came_ref[...].astype(F32)).astype(BF16)
                own_ref[...] = g[BG:]

            pltpu.emit_pipeline(body_x, grid=(FF // b,), in_specs=[by, single], out_specs=[single, single])(
                DG.at[layer, m], RC.at[i, 0], SX.at[i], OWN.at[i])
            send_x(i, False).start()

        pl.run_scoped(scoped, pltpu.VMEM((2 * BG, T), BF16))

    def grad_d(layer):
        b = 384
        n = BD // b
        row = pl.BlockSpec((b, D), lambda j: (j, 0))

        def hid_of(block):
            return pl.BlockSpec((T, b), lambda j: (0, block * n + j))

        def body(hid_ref, out_ref):
            out_ref[...] = tn(hid_ref[...], by_all[...]).astype(BF16)

        def body_x(hid_ref, came_ref, out_ref):
            g = tn(hid_ref[...], by_all[...]).astype(BF16)
            out_ref[...] = (g.astype(F32) + came_ref[...].astype(F32)).astype(BF16)

        def to_core(k, _):
            block = 2 * ((1 - xx) * (1 - k) + xx * k) + 1 - cc
            pltpu.emit_pipeline(body, grid=(n,), in_specs=[hid_of(block)], out_specs=[row])(HID.at[layer], SCD.at[layer, k])
            send_c(layer, k, True).start()
            return 0

        lax.fori_loop(0, 2, to_core, 0)
        send_c(layer, 0, True).wait_recv()
        pltpu.emit_pipeline(body_x, grid=(n,), in_specs=[hid_of(dx_), row], out_specs=[row])(HID.at[layer], RCD.at[layer, 0], SXD.at[layer])
        send_x(layer, True).start()
        pltpu.emit_pipeline(body, grid=(n,), in_specs=[hid_of(d)], out_specs=[row])(HID.at[layer], OWND.at[layer])

    def finish(i, is_d):
        send_x(i, is_d).wait_recv()
        send_c(i, 1, is_d).wait_recv()
        rows, cols, b, total = (BD, D, 384, tot_d) if is_d else (BG, FF, 96, tot_g)

        def body(own_ref, core_ref, came_ref, out_ref):
            g = (own_ref[...].astype(F32) + core_ref[...].astype(F32) + came_ref[...].astype(F32)).astype(BF16)
            out_ref[...] = g
            g = g.astype(F32)
            total[...] += jnp.sum((g * g).reshape(b // 8, 8, cols), axis=0)

        row = pl.BlockSpec((b, cols), lambda j: (j, 0))
        pipe = pltpu.emit_pipeline(body, grid=(rows // b,), in_specs=[row] * 3, out_specs=[row])
        if is_d:
            pipe(OWND.at[i], RCD.at[i, 1], RXD.at[i], gd.at[i])
        else:
            layer, m = i // 2, i % 2
            pl.when(m == 0)(lambda: pipe(OWN.at[i], RC.at[i, 1], RX.at[i], gg.at[layer]))
            pl.when(m == 1)(lambda: pipe(OWN.at[i], RC.at[i, 1], RX.at[i], gu.at[layer]))

    norm()
    on_y(Gate(0, 0))
    on_y(Gate(0, 1))
    on_c(Gate(0, 0))
    gate_up(0)
    on_c(Down(0, 0))
    on_y(Down(0, 1))
    on_c(Down(0, 1))
    on_y(Down(1, 0))
    whole(Down(0, 0))
    whole(Down(0, 1))
    begin(down_loads(0))
    end(down_loads(0))
    down()
    pltpu.make_async_copy(dy, by_all, by_sem).wait()
    whole(Down(1, 0))
    whole(Down(1, 1))
    begin(down_loads(1))
    by_hidden_1()
    gate_up(1)

    def backward(i, _):
        layer = 1 - i
        pl.when(i == 0)(lambda: begin(down_loads(0)))
        grad_d(layer)

        @pl.when(i == 1)
        def _():
            end(down_loads(0))
            by_hidden_0()

        def both(m, _):
            grad_gu(layer, m)
            return 0

        lax.fori_loop(0, 2, both, 0)
        pl.when(i == 0)(by_input)
        return 0

    lax.fori_loop(0, L, backward, 0)
    tot_g[...] = jnp.zeros_like(tot_g)
    tot_d[...] = jnp.zeros_like(tot_d)

    def finish_layer(n, _):
        layer = 1 - n
        finish(layer, True)

        def both(m, _):
            finish(2 * layer + m, False)
            return 0

        return lax.fori_loop(0, 2, both, 0)

    lax.fori_loop(0, L, finish_layer, 0)

    mine = tot_d[:, pl.ds(0, 128)]
    for n in range(1, D // 128):
        mine = mine + tot_d[:, pl.ds(n * 128, 128)]
    for n in range(FF // 128):
        mine = mine + tot_g[:, pl.ds(n * 128, 128)]
    sq_all[d] = mine
    exchange = [remote(sq_all.at[d], sq_all.at[d], sq_send.at[n], sq_recv.at[n], to) for n, to in enumerate((to_c, to_x, to_xc))]
    begin(exchange)
    for c in exchange:
        c.wait_recv()
    sq[...] = ((sq_all[0] + sq_all[1]) + sq_all[2]) + sq_all[3]
    for c in exchange:
        c.wait_send()

    for unit in every:
        for hop in range(4):
            for c in unit.copies(hop):
                c.wait_send()

    def sent(layer, _):
        for i, is_d in ((2 * layer, False), (2 * layer + 1, False), (layer, True)):
            send_c(i, 0, is_d).wait_send()
            send_c(i, 1, is_d).wait_send()
            send_x(i, is_d).wait_send()
        return 0

    lax.fori_loop(0, L, sent, 0)


def fused(x, dy, wg, wu, wd):
    def hbm(*shape, dtype=BF16):
        return jax.ShapeDtypeStruct(shape, dtype)

    outs = [
        hbm(L, BG, FF), hbm(L, BG, FF), hbm(L, BD, D), hbm(8, 128, dtype=F32),
        hbm(L, 2, D, FF), hbm(L, FF, D), hbm(L, D, T), hbm(T, D), hbm(L, T, FF), hbm(2, T, FF, dtype=F32), hbm(T, FF), hbm(L, 2, T, FF),
        hbm(4, 2, BG, FF), hbm(4, 2, BG, FF), hbm(4, BG, FF), hbm(4, BG, FF), hbm(4, BG, FF),
        hbm(2, 2, BD, D), hbm(2, 2, BD, D), hbm(2, BD, D), hbm(2, BD, D), hbm(2, BD, D),
    ]
    specs = [ANY] * len(outs)
    specs[3] = pl.BlockSpec(memory_space=pltpu.VMEM)
    dma = pltpu.SemaphoreType.DMA
    return pl.pallas_call(
        mega,
        out_shape=outs,
        in_specs=[ANY] * 5,
        out_specs=specs,
        scratch_shapes=[
            pltpu.VMEM((2, D, FF), BF16), pltpu.VMEM((FF, D), BF16), pltpu.VMEM((T, D), BF16), pltpu.VMEM((T, D), BF16),
            pltpu.VMEM((8, FF), F32), pltpu.VMEM((8, D), F32), pltpu.VMEM((4, 8, 128), F32),
            dma((L, NU, 2, 4)), dma((L, NU, 2, 4)), dma((L, 2, 4)), dma((L, 2, 4)), dma((6, 2)), dma((6, 2)), dma((6,)), dma((6,)),
            dma((3,)), dma((3,)), dma((2, 4)), dma((4,)), dma,
        ],
        compiler_params=pltpu.CompilerParams(collective_id=0, has_side_effects=True, vmem_limit_bytes=67043328),
        name="step",
    )(x, dy, wg, wu, wd)[:4]


def adamw(w, m, v, g):
    m = 0.9 * m + 0.1 * g
    v = 0.95 * v + 0.05 * g * g
    step = m * lax.rsqrt(v + 1e-8) + 0.1 * w
    return (w - 0.02 * step).astype(BF16), m, v


def solution(mesh):
    def step(x, dy, *arrays):
        weights, m, v = (arrays[i : i + 3] for i in (0, 3, 6))
        *gradients, sq = fused(x[0], dy[0], *weights)
        squares = jnp.sum(sq)
        count = lax.psum(1, "dp") * sum(g.size for g in gradients)
        factor = jnp.minimum(1.0, 0.5 * lax.rsqrt(squares / count + 1e-30))
        new = [adamw(w.astype(F32), m, v, g.astype(F32) * factor) for w, m, v, g in zip(weights, m, v, gradients, strict=True)]
        return tuple(one[which] for which in range(3) for one in new)

    states, cut = P(("rep", "dp"), None, None), P(None, "dp", None)
    return jax.shard_map(
        step,
        mesh=mesh,
        in_specs=(states, states) + (cut,) * 9,
        out_specs=(P("rep", "dp", None),) * 9,
        check_vma=False,
    )
```

```python
import jax
import jax.numpy as jnp
from jax import lax
from jax.experimental import pallas as pl
from jax.experimental.pallas import tpu as pltpu
from jax.sharding import PartitionSpec as P

MESH = pl.DeviceIdType.MESH
T, D, FF, L = 2048, 1152, 4608, 2
BG, BD = D // 4, FF // 4
FU = 768
NU = FF // FU
ND = 4
F32, BF16 = jnp.float32, jnp.bfloat16
ANY = pl.BlockSpec(memory_space=pl.ANY)


def nn(a, b):
    return lax.dot_general(a, b, (((1,), (0,)), ((), ())), preferred_element_type=F32)


def nt(a, b):
    return lax.dot_general(a, b, (((1,), (1,)), ((), ())), preferred_element_type=F32)


def tn(a, b):
    return lax.dot_general(a, b, (((0,), (0,)), ((), ())), preferred_element_type=F32)


def mega(x, dy, wg, wu, wd, *refs):
    (gg, gu, gd, sq, GU, WD, AT, H1, HID, PRE, DG, SG, RG, SD, RD) = refs[:15]
    (wgu, wdv, acts, tot_g, tot_d, sq_all) = refs[15:21]
    (gs, gr, ds_, dr, gcs, gcr, gxs, gxr, dcs, dcr, dxs, dxr, sq_send, sq_recv, load_sem, wd_sem, by_sem) = refs[21:]
    a_all = acts.at[0]
    r, d = lax.axis_index("rep"), lax.axis_index("dp")
    xx, cc = d // 2, d % 2
    dc, dx_, dxc = 2 * xx + 1 - cc, 2 * (1 - xx) + cc, 2 * (1 - xx) + 1 - cc
    to_c, to_x, to_xc, to_y = (r, dc), (r, dx_), (r, dxc), (1 - r, d)

    barrier = pltpu.get_barrier_semaphore()
    for to in (to_c, to_x, to_xc, to_y):
        pl.semaphore_signal(barrier, inc=1, device_id=to, device_id_type=MESH)
    pl.semaphore_wait(barrier, 4)

    def remote(src, dst, s, q, to):
        return pltpu.make_async_remote_copy(src_ref=src, dst_ref=dst, send_sem=s, recv_sem=q, device_id=to, device_id_type=MESH)

    def piece(arg, full, layer, block, r0, rows, cols, s, q, hop):
        half = rows // 2
        if hop == 0:
            mine = r0 + r * half
            return remote(arg.at[layer, pl.ds(mine, half), cols], full.at[pl.ds(d * block + mine, half), cols], s, q, to_x)
        if hop == 1:
            at = full.at[pl.ds(dx_ * block + r0 + r * half, half), cols]
            return remote(at, at, s, q, to_y)
        if hop == 2:
            return remote(arg.at[layer, pl.ds(r0, rows), cols], full.at[pl.ds(d * block + r0, rows), cols], s, q, to_c)
        at = full.at[pl.ds(dx_ * block + r0, rows), cols]
        return remote(at, at, s, q, to_c)

    def columns(u):
        return pl.ds(u * FU if isinstance(u, int) else pl.multiple_of(u * FU, FU), FU)

    class Gate:
        def __init__(self, layer, u):
            self.layer, self.u = layer, u

        def copies(self, hop):
            layer, u = self.layer, self.u
            return [piece(arg, GU.at[layer, m], layer, BG, 0, BG, columns(u), gs.at[layer, u, m, hop], gr.at[layer, u, m, hop], hop)
                    for m, arg in enumerate((wg, wu))]

    class Down:
        def __init__(self, layer, u):
            self.layer, self.u = layer, u

        def copies(self, hop):
            layer, u = self.layer, self.u
            return [piece(wd, WD.at[layer], layer, BD, u * (BD // ND), BD // ND, pl.ds(0, D), ds_.at[layer, u, hop], dr.at[layer, u, hop], hop)]

    def start(unit, hop):
        for c in unit.copies(hop):
            c.start()

    def arrive(unit, hop):
        for c in unit.copies(hop):
            c.wait_recv()

    def on_y(unit):
        arrive(unit, 0)
        start(unit, 1)

    def on_c(unit):
        arrive(unit, 1)
        start(unit, 3)

    def whole(unit):
        arrive(unit, 2)
        arrive(unit, 3)

    every = [unit(layer, u) for layer in range(L) for unit, n in ((Gate, NU), (Down, ND)) for u in range(n)]
    for unit in every:
        start(unit, 0)
    for unit in every:
        start(unit, 2)
    pltpu.make_async_copy(dy, acts.at[1], by_sem).start()

    def gate_loads(layer, u):
        out = []
        for m, arg in enumerate((wg, wu)):
            for i, b in enumerate((d, dc, dx_, dxc)):
                rows = pl.ds(b * BG, BG)
                src = GU.at[layer, m, rows, columns(u)] if i else arg.at[layer, :, columns(u)]
                out.append(pltpu.make_async_copy(src, wgu.at[m, rows, columns(u)], load_sem.at[m, i]))
        return out

    def down_loads(layer, u):
        out = []
        for i, b in enumerate((d, dc, dx_, dxc)):
            part = pl.ds(u * (BD // ND), BD // ND)
            rows = pl.ds(b * BD + u * (BD // ND), BD // ND)
            out.append(pltpu.make_async_copy(WD.at[layer, rows, :] if i else wd.at[layer, part, :], wdv.at[rows, :], wd_sem.at[i, u]))
        return out

    def all_down_loads(layer):
        return [c for u in range(ND) for c in down_loads(layer, u)]

    def begin(copies):
        for c in copies:
            c.start()

    def end(copies):
        for c in copies:
            c.wait()

    def begin_when(cases):
        for when, c in cases:
            if when is True:
                c.start()
            else:
                pl.when(when)(c.start)

    def end_when(cases):
        for when, c in cases:
            if when is True:
                c.wait()
            else:
                pl.when(when)(c.wait)

    def norm_of(h):
        wide = h.astype(F32)
        scale = lax.rsqrt(jnp.mean(wide * wide, -1, keepdims=True) + 1e-6)
        return wide * scale

    def rows_of(i, b):
        return pl.ds(pl.multiple_of(i * b, b), b)

    def at_steps(step, hooks):
        for when, what in hooks.items():

            @pl.when(step == when)
            def _(what=what):
                what()

    def norm():
        b = 512

        def body(x_ref, at_ref):
            a = norm_of(x_ref[...])
            a_all[rows_of(pl.program_id(0), b), :] = a.astype(BF16)
            at_ref[...] = a.T.astype(BF16)

        pltpu.emit_pipeline(
            body, grid=(T // b,), in_specs=[pl.BlockSpec((b, D), lambda i: (i, 0))], out_specs=[pl.BlockSpec((D, b), lambda i: (0, i))],
        )(x, AT.at[0])

    def gate_up(layer, hooks):
        b = 1024

        def body(gate_ref, up_ref, hid_ref):
            u, t = pl.program_id(0), pl.program_id(1)
            pl.when(t == 0)(lambda: end(gate_loads(layer, u)))
            at_steps(2 * u + t, hooks)
            a = a_all[rows_of(t, b), :]

            @pl.when((t == 1) & (u + 1 < NU))
            def _():
                whole(Gate(layer, u + 1))
                begin(gate_loads(layer, u + 1))

            gate = nn(a, wgu[0, :, columns(u)])
            gate_ref[...] = gate
            up = nn(a, wgu[1, :, columns(u)])
            up_ref[...] = up
            hid_ref[...] = (gate * jax.nn.sigmoid(gate) * up).astype(BF16)

        tile = pl.BlockSpec((b, FU), lambda u, t: (t, u))
        pltpu.emit_pipeline(body, grid=(NU, T // b), in_specs=[], out_specs=[tile] * 3)(PRE.at[layer, 0], PRE.at[layer, 1], HID.at[layer])

    def down():
        b = 256

        def body(x_ref, hid_ref, h_ref, at_ref):
            i = pl.program_id(0)
            at_steps(i, {
                2: lambda: on_y(Gate(1, 1)),
                3: lambda: on_c(Gate(1, 0)),
                5: lambda: (on_y(Gate(1, 2)), on_c(Gate(1, 1))),
                7: lambda: (on_y(Gate(1, 3)), whole(Gate(1, 0)), begin(gate_loads(1, 0))),
            })
            h = x_ref[...] + nn(hid_ref[...], wdv[...]).astype(BF16)
            h_ref[...] = h
            a = norm_of(h)
            a_all[rows_of(i, b), :] = a.astype(BF16)
            at_ref[...] = a.T.astype(BF16)

        row = pl.BlockSpec((b, D), lambda i: (i, 0))
        pltpu.emit_pipeline(
            body, grid=(T // b,), in_specs=[row, pl.BlockSpec((b, FF), lambda i: (i, 0))],
            out_specs=[row, pl.BlockSpec((D, b), lambda i: (0, i))],
        )(x, HID.at[0], H1, AT.at[1])

    def by_hidden(layer):
        b, n = 512, 1152

        def body(gate_ref, up_ref, bg_ref, bu_ref):
            i, j = pl.program_id(0), pl.program_id(1)
            by_hid = nt(acts[layer, rows_of(i, b), :], wdv[rows_of(j, n), :]).astype(BF16).astype(F32)
            gate, up = gate_ref[...], up_ref[...]
            s = jax.nn.sigmoid(gate)
            silu = gate * s
            bu_ref[...] = (by_hid * silu).astype(BF16)
            bg_ref[...] = (by_hid * up * (s + silu * (1 - s))).astype(BF16)

        deep = pl.BlockSpec((b, n), lambda i, j: (i, j), pipeline_mode=pl.Buffered(3))
        tile = pl.BlockSpec((b, n), lambda i, j: (i, j))
        pltpu.emit_pipeline(body, grid=(T // b, FF // n), in_specs=[deep, deep], out_specs=[tile, tile])(
            PRE.at[layer, 0], PRE.at[layer, 1], DG.at[layer, 0], DG.at[layer, 1])

    def by_input():
        b = 256

        def body(bg_ref, bu_ref, h_ref):
            rows = rows_of(pl.program_id(0), b)
            by_a = nt(bg_ref[...], wgu[0]).astype(BF16).astype(F32) + nt(bu_ref[...], wgu[1]).astype(BF16).astype(F32)
            by_a = by_a.astype(BF16).astype(F32)
            wide = h_ref[...].astype(F32)
            scale = lax.rsqrt(jnp.mean(wide * wide, -1, keepdims=True) + 1e-6)
            along = jnp.mean(by_a * wide, -1, keepdims=True)
            by_h = by_a * scale - wide * (scale * scale * scale * along)
            acts[0, rows, :] = acts[1, rows, :] + by_h.astype(BF16)

        row, wide_row = pl.BlockSpec((b, D), lambda i: (i, 0)), pl.BlockSpec((b, FF), lambda i: (i, 0))
        pltpu.emit_pipeline(body, grid=(T // b,), in_specs=[wide_row, wide_row, row], out_specs=[])(DG.at[1, 0], DG.at[1, 1], H1)

    def block_of(k):
        return 2 * ((1 - xx) * (1 - k // 2) + xx * (k // 2)) + (1 - cc) * (1 - k % 2) + cc * (k % 2)

    BT, BC = 384, 768
    DT, GT = BD // BT, FF // BC

    def d_rows(j):
        return pl.ds(pl.multiple_of(j * BT, BT), BT)

    def d_core(layer, p, j):
        at = (layer, 2 * p, d_rows(j), slice(None))
        return remote(SD.at[at], RD.at[at], dcs.at[layer, p, j], dcr.at[layer, p, j], to_c)

    def d_x(layer, j):
        at = (layer, 1, d_rows(j), slice(None))
        return remote(SD.at[at], RD.at[at], dxs.at[layer, j], dxr.at[layer, j], to_x)

    def g_cols(j):
        return pl.ds(pl.multiple_of(j * BC, BC), BC)

    def g_core(i, p, j):
        at = (i, 2 * p, slice(None), g_cols(j))
        return remote(SG.at[at], RG.at[at], gcs.at[i, p, j], gcr.at[i, p, j], to_c)

    def g_x(i, j):
        at = (i, 1, slice(None), g_cols(j))
        return remote(SG.at[at], RG.at[at], gxs.at[i, j], gxr.at[i, j], to_x)

    def square(total, g, cols):
        g = g.astype(F32)
        total[...] += jnp.sum((g * g).reshape(g.shape[0] // 8, 8, cols), axis=0)

    def grad_d(layer, p):
        def scoped(made, came, made_sem, came_sem):
            def to_hbm(n):
                def copy(dst):
                    return pltpu.make_async_copy(made.at[n % 2], dst, made_sem.at[n % 2])

                stage = copy(SD.at[layer, 2 * p + n // DT * (1 - p), d_rows(n % DT), :])
                return [(n < DT, stage), (n >= DT, copy(gd.at[layer, d_rows(n % DT), :]))] if p else [(True, stage)]

            def from_hbm(j, k):
                src = RD.at[layer, 1 if k else 2 * p, d_rows(j), :]
                return pltpu.make_async_copy(src, came.at[j % 2, k], came_sem.at[j % 2, k])

            def fetch(j):
                d_core(layer, p, j).wait_recv()
                from_hbm(j, 0).start()
                if p:
                    d_x(layer, j).wait_recv()
                    from_hbm(j, 1).start()

            def send(n):
                end_when(to_hbm(n))
                pl.when(n < DT)(lambda: d_core(layer, p, n % DT).start())
                if p == 0:
                    pl.when(n >= DT)(lambda: d_x(layer, n % DT).start())

            def body(hid_ref):
                n = pl.program_id(0)
                if p == 0:
                    pl.when((layer == 1) & (n == 3))(lambda: on_c(Down(1, 3)))

                    @pl.when((layer == 1) & (n == 5))
                    def _():
                        for u in range(ND):
                            whole(Down(1, u))
                        begin(all_down_loads(1))

                made[n % 2] = tn(hid_ref[...], acts[layer]).astype(BF16)

                @pl.when(n >= DT)
                def _():
                    j = n % DT
                    from_hbm(j, 0).wait()
                    g = made[n % 2].astype(F32) + came[j % 2, 0].astype(F32)
                    if p:
                        from_hbm(j, 1).wait()
                        g = g + came[j % 2, 1].astype(F32)
                    g = g.astype(BF16)
                    made[n % 2] = g
                    if p:
                        square(tot_d, g, D)

                begin_when(to_hbm(n))
                pl.when(n > 0)(lambda: send(n - 1))
                pl.when((n >= DT - 1) & (n < 2 * DT - 1))(lambda: fetch(n - (DT - 1)))

            hid = pl.BlockSpec((T, BT), lambda n: (0, block_of(2 * p + n // DT) * DT + n % DT))
            pltpu.emit_pipeline(body, grid=(2 * DT,), in_specs=[hid], out_specs=[])(HID.at[layer])
            send(2 * DT - 1)

        dma = pltpu.SemaphoreType.DMA
        pl.run_scoped(scoped, pltpu.VMEM((2, BT, D), BF16), pltpu.VMEM((2, 1 + p, BT, D), BF16), dma((2,)), dma((2, 2)))

    def grad_gu(layer, p):
        steps = 2 * GT

        def scoped(lhs, made, came, made_sem, own_sem, came_sem):
            rows = [
                pltpu.make_async_copy(AT.at[layer, pl.ds(block_of(2 * p + h) * BG, BG), :], lhs.at[pl.ds(h * BG, BG), :], load_sem.at[0, h])
                for h in range(2)
            ]

            def to_hbm(q, h):
                m, cols = q // GT, g_cols(q % GT)

                def copy(dst):
                    return pltpu.make_async_copy(made.at[q % 4, h], dst, (made_sem, own_sem)[h].at[q % 4])

                if p and h:
                    return [(m == 0, copy(gg.at[layer, :, cols])), (m == 1, copy(gu.at[layer, :, cols]))]
                return [(True, copy(SG.at[2 * layer + m, 2 * p + h, :, cols]))]

            def from_hbm(q, k):
                src = RG.at[2 * layer + q // GT, 1 if k else 2 * p, :, g_cols(q % GT)]
                return pltpu.make_async_copy(src, came.at[q % 2, k], came_sem.at[q % 2, k])

            def stage_1(q):
                end_when(to_hbm(q, 0))
                g_core(2 * layer + q // GT, p, q % GT).start()

            def stage_2(q):
                i, j = 2 * layer + q // GT, q % GT
                g_core(i, p, j).wait_recv()
                from_hbm(q, 0).start()
                if p:
                    g_x(i, j).wait_recv()
                    from_hbm(q, 1).start()

            def stage_3(q):
                from_hbm(q, 0).wait()
                g = made[q % 4, 1].astype(F32) + came[q % 2, 0].astype(F32)
                if p:
                    from_hbm(q, 1).wait()
                    g = g + came[q % 2, 1].astype(F32)
                g = g.astype(BF16)
                made[q % 4, 1] = g
                if p:
                    square(tot_g, g, BC)
                begin_when(to_hbm(q, 1))

            def stage_4(q):
                end_when(to_hbm(q, 1))
                if p == 0:
                    g_x(2 * layer + q // GT, q % GT).start()

            def stage(q, late):
                what = (stage_1, stage_2, stage_3, stage_4)[late - 1]
                pl.when((q >= late) & (q < steps + late))(lambda: what(q - late))

            begin(rows)

            def body(by_ref):
                q = GT * pl.program_id(0) + pl.program_id(1)
                pl.when(q == 0)(lambda: end(rows))
                stage(q, 4)
                g = nn(lhs[...], by_ref[0]).astype(BF16)
                made[q % 4, 0] = g[:BG]
                made[q % 4, 1] = g[BG:]
                for late in (3, 2, 1):
                    stage(q, late)
                begin_when(to_hbm(q, 0))

            by = pl.BlockSpec((1, T, BC), lambda m, n: (m, 0, n))
            pltpu.emit_pipeline(body, grid=(2, GT), in_specs=[by], out_specs=[])(DG.at[layer])

            def drain(n, _):
                for late in (4, 3, 2, 1):
                    stage(steps + n, late)
                return 0

            lax.fori_loop(0, 4, drain, 0)

        four, two = pltpu.SemaphoreType.DMA((4,)), pltpu.SemaphoreType.DMA((2, 2))
        pl.run_scoped(
            scoped, pltpu.VMEM((2 * BG, T), BF16), pltpu.VMEM((4, 2, BG, BC), BF16), pltpu.VMEM((2, 1 + p, BG, BC), BF16), four, four, two)

    norm()
    on_y(Gate(0, 0))
    on_y(Gate(0, 1))
    on_c(Gate(0, 0))
    whole(Gate(0, 0))
    begin(gate_loads(0, 0))
    hooks = {2 * u: lambda u=u: (on_y(Gate(0, u + 2)), on_c(Gate(0, u + 1))) for u in range(NU - 2)}
    hooks |= {
        7: lambda: on_y(Down(0, 0)),
        8: lambda: (on_y(Down(0, 1)), on_c(Gate(0, 5))),
        9: lambda: (on_y(Down(0, 2)), on_c(Down(0, 0))),
        10: lambda: (on_y(Down(0, 3)), on_c(Down(0, 1))),
        11: lambda: on_c(Down(0, 2)),
    }
    gate_up(0, hooks)
    whole(Down(0, 0))
    begin(down_loads(0, 0))
    whole(Down(0, 1))
    begin(down_loads(0, 1))
    whole(Down(0, 2))
    begin(down_loads(0, 2))
    on_c(Down(0, 3))
    on_y(Gate(1, 0))
    whole(Down(0, 3))
    begin(down_loads(0, 3))
    end(all_down_loads(0))
    down()
    hooks = {
        0: lambda: on_c(Gate(1, 2)),
        1: lambda: on_y(Gate(1, 4)),
        2: lambda: on_c(Gate(1, 3)),
        3: lambda: on_y(Gate(1, 5)),
        4: lambda: on_c(Gate(1, 4)),
        5: lambda: on_y(Down(1, 0)),
        6: lambda: on_c(Gate(1, 5)),
        7: lambda: (on_y(Down(1, 1)), on_c(Down(1, 0))),
        9: lambda: (on_y(Down(1, 2)), on_c(Down(1, 1))),
        11: lambda: (on_y(Down(1, 3)), on_c(Down(1, 2))),
    }
    gate_up(1, hooks)
    pltpu.make_async_copy(dy, acts.at[1], by_sem).wait()

    def backward(i, _):
        layer = 1 - i
        grad_d(layer, 0)
        end(all_down_loads(layer))
        by_hidden(layer)
        pl.when(i == 0)(lambda: begin(all_down_loads(0)))
        grad_gu(layer, 0)
        pl.when(i == 0)(by_input)
        return 0

    lax.fori_loop(0, L, backward, 0)

    tot_g[...] = jnp.zeros_like(tot_g)
    tot_d[...] = jnp.zeros_like(tot_d)

    def rest(i, _):
        grad_d(1 - i, 1)
        grad_gu(1 - i, 1)
        return 0

    lax.fori_loop(0, L, rest, 0)
    mine = tot_d[:, pl.ds(0, 128)]
    for n in range(1, D // 128):
        mine = mine + tot_d[:, pl.ds(n * 128, 128)]
    for n in range(BC // 128):
        mine = mine + tot_g[:, pl.ds(n * 128, 128)]
    sq_all[d] = mine
    exchange = [remote(sq_all.at[d], sq_all.at[d], sq_send.at[n], sq_recv.at[n], to) for n, to in enumerate((to_c, to_x, to_xc))]
    begin(exchange)
    for c in exchange:
        c.wait_recv()
    sq[...] = ((sq_all[0] + sq_all[1]) + sq_all[2]) + sq_all[3]
    for c in exchange:
        c.wait_send()

    for unit in every:
        for hop in range(4):
            for c in unit.copies(hop):
                c.wait_send()

    def sent(layer, _):
        for j in range(DT):
            for c in (d_core(layer, 0, j), d_core(layer, 1, j), d_x(layer, j)):
                c.wait_send()
        for m in range(2):
            for j in range(GT):
                g_core(2 * layer + m, 0, j).wait_send()
                g_core(2 * layer + m, 1, j).wait_send()
                g_x(2 * layer + m, j).wait_send()
        return 0

    lax.fori_loop(0, L, sent, 0)


def fused(x, dy, wg, wu, wd):
    def hbm(*shape, dtype=BF16):
        return jax.ShapeDtypeStruct(shape, dtype)

    outs = [
        hbm(L, BG, FF), hbm(L, BG, FF), hbm(L, BD, D), hbm(8, 128, dtype=F32),
        hbm(L, 2, D, FF), hbm(L, FF, D), hbm(L, D, T), hbm(T, D), hbm(L, T, FF), hbm(L, 2, T, FF, dtype=F32), hbm(L, 2, T, FF),
        hbm(4, 3, BG, FF), hbm(4, 3, BG, FF), hbm(2, 3, BD, D), hbm(2, 3, BD, D),
    ]
    specs = [ANY] * len(outs)
    specs[3] = pl.BlockSpec(memory_space=pltpu.VMEM)
    dma = pltpu.SemaphoreType.DMA
    return pl.pallas_call(
        mega,
        out_shape=outs,
        in_specs=[ANY] * 5,
        out_specs=specs,
        scratch_shapes=[
            pltpu.VMEM((2, D, FF), BF16), pltpu.VMEM((FF, D), BF16), pltpu.VMEM((2, T, D), BF16),
            pltpu.VMEM((8, FU), F32), pltpu.VMEM((8, D), F32), pltpu.VMEM((4, 8, 128), F32),
            dma((L, NU, 2, 4)), dma((L, NU, 2, 4)), dma((L, ND, 4)), dma((L, ND, 4)), dma((4, 2, 6)), dma((4, 2, 6)), dma((4, 6)), dma((4, 6)),
            dma((L, 2, 3)), dma((L, 2, 3)), dma((L, 3)), dma((L, 3)), dma((3,)), dma((3,)), dma((2, 4)), dma((4, ND)), dma,
        ],
        compiler_params=pltpu.CompilerParams(collective_id=0, has_side_effects=True, vmem_limit_bytes=67043328),
        name="step",
    )(x, dy, wg, wu, wd)[:4]


def adamw(w, m, v, g):
    m = 0.9 * m + 0.1 * g
    v = 0.95 * v + 0.05 * g * g
    step = m * lax.rsqrt(v + 1e-8) + 0.1 * w
    return (w - 0.02 * step).astype(BF16), m, v


def solution(mesh):
    def step(x, dy, *arrays):
        weights, m, v = (arrays[i : i + 3] for i in (0, 3, 6))
        *gradients, sq = fused(x[0], dy[0], *weights)
        squares = jnp.sum(sq)
        count = lax.psum(1, "dp") * sum(g.size for g in gradients)
        factor = jnp.minimum(1.0, 0.5 * lax.rsqrt(squares / count + 1e-30))
        new = [adamw(w.astype(F32), m, v, g.astype(F32) * factor) for w, m, v, g in zip(weights, m, v, gradients, strict=True)]
        return tuple(one[which] for which in range(3) for one in new)

    states, cut = P(("rep", "dp"), None, None), P(None, "dp", None)
    return jax.shard_map(
        step,
        mesh=mesh,
        in_specs=(states, states) + (cut,) * 9,
        out_specs=(P("rep", "dp", None),) * 9,
        check_vma=False,
    )
```

```python
import jax
import jax.numpy as jnp
from jax import lax
from jax.experimental import pallas as pl
from jax.experimental.pallas import tpu as pltpu
from jax.sharding import PartitionSpec as P

MESH = pl.DeviceIdType.MESH
T, D, FF, L = 2048, 1152, 4608, 2
BG, BD = D // 4, FF // 4
FU = 768
NU = FF // FU
ND = 4
F32, BF16 = jnp.float32, jnp.bfloat16
ANY = pl.BlockSpec(memory_space=pl.ANY)


def nn(a, b):
    return lax.dot_general(a, b, (((1,), (0,)), ((), ())), preferred_element_type=F32)


def nt(a, b):
    return lax.dot_general(a, b, (((1,), (1,)), ((), ())), preferred_element_type=F32)


def tn(a, b):
    return lax.dot_general(a, b, (((0,), (0,)), ((), ())), preferred_element_type=F32)


def mega(x, dy, wg, wu, wd, *refs):
    (gg, gu, gd, sq, GU, WD, AT, H1, HID, PRE, DG, SG, RG, SD, RD) = refs[:15]
    (wgu, wdv, acts, tot_g, tot_d, sq_all) = refs[15:21]
    (gs, gr, ds_, dr, gcs, gcr, gxs, gxr, dcs, dcr, dxs, dxr, sq_send, sq_recv, load_sem, wd_sem, by_sem) = refs[21:]
    a_all = acts.at[0]
    r, d = lax.axis_index("rep"), lax.axis_index("dp")
    xx, cc = d // 2, d % 2
    dc, dx_, dxc = 2 * xx + 1 - cc, 2 * (1 - xx) + cc, 2 * (1 - xx) + 1 - cc
    to_c, to_x, to_xc, to_y = (r, dc), (r, dx_), (r, dxc), (1 - r, d)

    barrier = pltpu.get_barrier_semaphore()
    for to in (to_c, to_x, to_xc, to_y):
        pl.semaphore_signal(barrier, inc=1, device_id=to, device_id_type=MESH)
    pl.semaphore_wait(barrier, 4)

    def remote(src, dst, s, q, to):
        return pltpu.make_async_remote_copy(src_ref=src, dst_ref=dst, send_sem=s, recv_sem=q, device_id=to, device_id_type=MESH)

    def piece(arg, full, layer, block, r0, rows, cols, s, q, hop):
        half = rows // 2
        if hop == 0:
            mine = r0 + r * half
            return remote(arg.at[layer, pl.ds(mine, half), cols], full.at[pl.ds(d * block + mine, half), cols], s, q, to_x)
        if hop == 1:
            at = full.at[pl.ds(dx_ * block + r0 + r * half, half), cols]
            return remote(at, at, s, q, to_y)
        if hop == 2:
            return remote(arg.at[layer, pl.ds(r0, rows), cols], full.at[pl.ds(d * block + r0, rows), cols], s, q, to_c)
        at = full.at[pl.ds(dx_ * block + r0, rows), cols]
        return remote(at, at, s, q, to_c)

    def columns(u):
        return pl.ds(u * FU if isinstance(u, int) else pl.multiple_of(u * FU, FU), FU)

    class Gate:
        def __init__(self, layer, u):
            self.layer, self.u = layer, u

        def copies(self, hop):
            layer, u = self.layer, self.u
            return [piece(arg, GU.at[layer, m], layer, BG, 0, BG, columns(u), gs.at[layer, u, m, hop], gr.at[layer, u, m, hop], hop)
                    for m, arg in enumerate((wg, wu))]

    class Down:
        def __init__(self, layer, u):
            self.layer, self.u = layer, u

        def copies(self, hop):
            layer, u = self.layer, self.u
            return [piece(wd, WD.at[layer], layer, BD, u * (BD // ND), BD // ND, pl.ds(0, D), ds_.at[layer, u, hop], dr.at[layer, u, hop], hop)]

    def start(unit, hop):
        for c in unit.copies(hop):
            c.start()

    def arrive(unit, hop):
        for c in unit.copies(hop):
            c.wait_recv()

    def on_y(unit):
        arrive(unit, 0)
        start(unit, 1)

    def on_c(unit):
        arrive(unit, 1)
        start(unit, 3)

    def whole(unit):
        arrive(unit, 2)
        arrive(unit, 3)

    every = [unit(layer, u) for layer in range(L) for unit, n in ((Gate, NU), (Down, ND)) for u in range(n)]
    for unit in every:
        start(unit, 0)
    for unit in every:
        start(unit, 2)
    pltpu.make_async_copy(dy, acts.at[1], by_sem).start()

    def gate_loads(layer, u):
        out = []
        for m, arg in enumerate((wg, wu)):
            for i, b in enumerate((d, dc, dx_, dxc)):
                rows = pl.ds(b * BG, BG)
                src = GU.at[layer, m, rows, columns(u)] if i else arg.at[layer, :, columns(u)]
                out.append(pltpu.make_async_copy(src, wgu.at[m, rows, columns(u)], load_sem.at[m, i]))
        return out

    def down_loads(layer, u):
        out = []
        for i, b in enumerate((d, dc, dx_, dxc)):
            part = pl.ds(u * (BD // ND), BD // ND)
            rows = pl.ds(b * BD + u * (BD // ND), BD // ND)
            out.append(pltpu.make_async_copy(WD.at[layer, rows, :] if i else wd.at[layer, part, :], wdv.at[rows, :], wd_sem.at[i, u]))
        return out

    def all_down_loads(layer):
        return [c for u in range(ND) for c in down_loads(layer, u)]

    def begin(copies):
        for c in copies:
            c.start()

    def end(copies):
        for c in copies:
            c.wait()

    def begin_when(cases):
        for when, c in cases:
            if when is True:
                c.start()
            else:
                pl.when(when)(c.start)

    def end_when(cases):
        for when, c in cases:
            if when is True:
                c.wait()
            else:
                pl.when(when)(c.wait)

    def norm_of(h):
        wide = h.astype(F32)
        scale = lax.rsqrt(jnp.mean(wide * wide, -1, keepdims=True) + 1e-6)
        return wide * scale

    def rows_of(i, b):
        return pl.ds(pl.multiple_of(i * b, b), b)

    def at_steps(step, hooks):
        for when, what in hooks.items():

            @pl.when(step == when)
            def _(what=what):
                what()

    def norm():
        b = 512

        def body(x_ref, at_ref):
            a = norm_of(x_ref[...])
            a_all[rows_of(pl.program_id(0), b), :] = a.astype(BF16)
            at_ref[...] = a.T.astype(BF16)

        pltpu.emit_pipeline(
            body, grid=(T // b,), in_specs=[pl.BlockSpec((b, D), lambda i: (i, 0))], out_specs=[pl.BlockSpec((D, b), lambda i: (0, i))],
        )(x, AT.at[0])

    def gate_up(layer, hooks):
        b = 1024

        def body(gate_ref, up_ref, hid_ref):
            u, t = pl.program_id(0), pl.program_id(1)
            pl.when(t == 0)(lambda: end(gate_loads(layer, u)))
            at_steps(2 * u + t, hooks)
            a = a_all[rows_of(t, b), :]

            @pl.when((t == 1) & (u + 1 < NU))
            def _():
                whole(Gate(layer, u + 1))
                begin(gate_loads(layer, u + 1))

            gate = nn(a, wgu[0, :, columns(u)])
            gate_ref[...] = gate
            up = nn(a, wgu[1, :, columns(u)])
            up_ref[...] = up
            hid_ref[...] = (gate * jax.nn.sigmoid(gate) * up).astype(BF16)

        tile = pl.BlockSpec((b, FU), lambda u, t: (t, u))
        pltpu.emit_pipeline(body, grid=(NU, T // b), in_specs=[], out_specs=[tile] * 3)(PRE.at[layer, 0], PRE.at[layer, 1], HID.at[layer])

    def down():
        b = 256

        def body(x_ref, hid_ref, h_ref, at_ref):
            i = pl.program_id(0)
            at_steps(i, {
                2: lambda: on_y(Gate(1, 1)),
                3: lambda: on_c(Gate(1, 0)),
                5: lambda: (on_y(Gate(1, 2)), on_c(Gate(1, 1))),
                7: lambda: (on_y(Gate(1, 3)), whole(Gate(1, 0)), begin(gate_loads(1, 0))),
            })
            h = x_ref[...] + nn(hid_ref[...], wdv[...]).astype(BF16)
            h_ref[...] = h
            a = norm_of(h)
            a_all[rows_of(i, b), :] = a.astype(BF16)
            at_ref[...] = a.T.astype(BF16)

        row = pl.BlockSpec((b, D), lambda i: (i, 0))
        pltpu.emit_pipeline(
            body, grid=(T // b,), in_specs=[row, pl.BlockSpec((b, FF), lambda i: (i, 0))],
            out_specs=[row, pl.BlockSpec((D, b), lambda i: (0, i))],
        )(x, HID.at[0], H1, AT.at[1])

    def by_hidden(layer):
        b, n = 512, 1152

        def body(gate_ref, up_ref, bg_ref, bu_ref):
            i, j = pl.program_id(0), pl.program_id(1)
            by_hid = nt(acts[layer, rows_of(i, b), :], wdv[rows_of(j, n), :]).astype(BF16).astype(F32)
            gate, up = gate_ref[...], up_ref[...]
            s = jax.nn.sigmoid(gate)
            silu = gate * s
            bu_ref[...] = (by_hid * silu).astype(BF16)
            bg_ref[...] = (by_hid * up * (s + silu * (1 - s))).astype(BF16)

        deep = pl.BlockSpec((b, n), lambda i, j: (i, j), pipeline_mode=pl.Buffered(3))
        tile = pl.BlockSpec((b, n), lambda i, j: (i, j))
        pltpu.emit_pipeline(body, grid=(T // b, FF // n), in_specs=[deep, deep], out_specs=[tile, tile])(
            PRE.at[layer, 0], PRE.at[layer, 1], DG.at[layer, 0], DG.at[layer, 1])

    def by_input():
        b = 256

        def body(bg_ref, bu_ref, h_ref):
            rows = rows_of(pl.program_id(0), b)
            by_a = nt(bg_ref[...], wgu[0]).astype(BF16).astype(F32) + nt(bu_ref[...], wgu[1]).astype(BF16).astype(F32)
            by_a = by_a.astype(BF16).astype(F32)
            wide = h_ref[...].astype(F32)
            scale = lax.rsqrt(jnp.mean(wide * wide, -1, keepdims=True) + 1e-6)
            along = jnp.mean(by_a * wide, -1, keepdims=True)
            by_h = by_a * scale - wide * (scale * scale * scale * along)
            acts[0, rows, :] = acts[1, rows, :] + by_h.astype(BF16)

        row, wide_row = pl.BlockSpec((b, D), lambda i: (i, 0)), pl.BlockSpec((b, FF), lambda i: (i, 0))
        pltpu.emit_pipeline(body, grid=(T // b,), in_specs=[wide_row, wide_row, row], out_specs=[])(DG.at[1, 0], DG.at[1, 1], H1)

    def block_of(k):
        return 2 * ((1 - xx) * (1 - k // 2) + xx * (k // 2)) + (1 - cc) * (1 - k % 2) + cc * (k % 2)

    BT, BC = 384, 768
    DT, GT, SLOTS = BD // BT, FF // BC, 5

    def d_rows(j):
        return pl.ds(pl.multiple_of(j * BT, BT), BT)

    def d_core(layer, p, j):
        at = (layer, 2 * p, d_rows(j), slice(None))
        return remote(SD.at[at], RD.at[at], dcs.at[layer, p, j], dcr.at[layer, p, j], to_c)

    def d_x(layer, j):
        at = (layer, 1, d_rows(j), slice(None))
        return remote(SD.at[at], RD.at[at], dxs.at[layer, j], dxr.at[layer, j], to_x)

    def g_cols(j):
        return pl.ds(pl.multiple_of(j * BC, BC), BC)

    def g_core(i, p, j):
        at = (i, 2 * p, slice(None), g_cols(j))
        return remote(SG.at[at], RG.at[at], gcs.at[i, p, j], gcr.at[i, p, j], to_c)

    def g_x(i, j):
        at = (i, 1, slice(None), g_cols(j))
        return remote(SG.at[at], RG.at[at], gxs.at[i, j], gxr.at[i, j], to_x)

    def square(total, g, cols):
        g = g.astype(F32)
        total[...] += jnp.sum((g * g).reshape(g.shape[0] // 8, 8, cols), axis=0)

    def grad_d(layer, p):
        def scoped(made, came, made_sem, came_sem):
            def to_hbm(n):
                def copy(dst):
                    return pltpu.make_async_copy(made.at[n % 2], dst, made_sem.at[n % 2])

                stage = copy(SD.at[layer, 2 * p + n // DT * (1 - p), d_rows(n % DT), :])
                return [(n < DT, stage), (n >= DT, copy(gd.at[layer, d_rows(n % DT), :]))] if p else [(True, stage)]

            def from_hbm(j, k):
                src = RD.at[layer, 1 if k else 2 * p, d_rows(j), :]
                return pltpu.make_async_copy(src, came.at[j % 2, k], came_sem.at[j % 2, k])

            def fetch(j):
                d_core(layer, p, j).wait_recv()
                from_hbm(j, 0).start()
                if p:
                    d_x(layer, j).wait_recv()
                    from_hbm(j, 1).start()

            def send(n):
                end_when(to_hbm(n))
                pl.when(n < DT)(lambda: d_core(layer, p, n % DT).start())
                if p == 0:
                    pl.when(n >= DT)(lambda: d_x(layer, n % DT).start())

            def body(hid_ref):
                n = pl.program_id(0)
                if p == 0:
                    pl.when((layer == 1) & (n == 3))(lambda: on_c(Down(1, 3)))

                    @pl.when((layer == 1) & (n == 5))
                    def _():
                        for u in range(ND):
                            whole(Down(1, u))
                        begin(all_down_loads(1))

                made[n % 2] = tn(hid_ref[...], acts[layer]).astype(BF16)

                @pl.when(n >= DT)
                def _():
                    j = n % DT
                    from_hbm(j, 0).wait()
                    g = made[n % 2].astype(F32) + came[j % 2, 0].astype(F32)
                    if p:
                        from_hbm(j, 1).wait()
                        g = g + came[j % 2, 1].astype(F32)
                    g = g.astype(BF16)
                    made[n % 2] = g
                    if p:
                        square(tot_d, g, D)

                begin_when(to_hbm(n))
                pl.when(n > 0)(lambda: send(n - 1))
                pl.when((n >= DT - 1) & (n < 2 * DT - 1))(lambda: fetch(n - (DT - 1)))

            hid = pl.BlockSpec((T, BT), lambda n: (0, block_of(2 * p + n // DT) * DT + n % DT))
            pltpu.emit_pipeline(body, grid=(2 * DT,), in_specs=[hid], out_specs=[])(HID.at[layer])
            send(2 * DT - 1)

        dma = pltpu.SemaphoreType.DMA
        pl.run_scoped(scoped, pltpu.VMEM((2, BT, D), BF16), pltpu.VMEM((2, 1 + p, BT, D), BF16), dma((2,)), dma((2, 2)))

    def grad_gu(layer, p):
        steps = 2 * GT

        def scoped(lhs, made, came, made_sem, own_sem, came_sem):
            rows = [
                pltpu.make_async_copy(AT.at[layer, pl.ds(block_of(2 * p + h) * BG, BG), :], lhs.at[pl.ds(h * BG, BG), :], load_sem.at[0, h])
                for h in range(2)
            ]

            def to_hbm(q, h):
                m, cols = q // GT, g_cols(q % GT)

                def copy(dst):
                    return pltpu.make_async_copy(made.at[q % SLOTS, h], dst, (made_sem, own_sem)[h].at[q % SLOTS])

                if p and h:
                    return [(m == 0, copy(gg.at[layer, :, cols])), (m == 1, copy(gu.at[layer, :, cols]))]
                return [(True, copy(SG.at[2 * layer + m, 2 * p + h, :, cols]))]

            def from_hbm(q, k):
                src = RG.at[2 * layer + q // GT, 1 if k else 2 * p, :, g_cols(q % GT)]
                return pltpu.make_async_copy(src, came.at[q % 2, k], came_sem.at[q % 2, k])

            def stage_1(q):
                end_when(to_hbm(q, 0))
                g_core(2 * layer + q // GT, p, q % GT).start()

            def stage_2(q):
                i, j = 2 * layer + q // GT, q % GT
                g_core(i, p, j).wait_recv()
                from_hbm(q, 0).start()
                if p:
                    g_x(i, j).wait_recv()
                    from_hbm(q, 1).start()

            def stage_3(q):
                from_hbm(q, 0).wait()
                g = made[q % SLOTS, 1].astype(F32) + came[q % 2, 0].astype(F32)
                if p:
                    from_hbm(q, 1).wait()
                    g = g + came[q % 2, 1].astype(F32)
                g = g.astype(BF16)
                made[q % SLOTS, 1] = g
                if p:
                    square(tot_g, g, BC)
                begin_when(to_hbm(q, 1))

            def stage_4(q):
                end_when(to_hbm(q, 1))
                if p == 0:
                    g_x(2 * layer + q // GT, q % GT).start()

            def stage(q, late):
                what = (stage_1, stage_2, stage_3, stage_4)[late - 1]
                pl.when((q >= late) & (q < steps + late))(lambda: what(q - late))

            begin(rows)

            def body(by_ref):
                q = GT * pl.program_id(0) + pl.program_id(1)
                pl.when(q == 0)(lambda: end(rows))
                g = nn(lhs[...], by_ref[0]).astype(BF16)
                made[q % SLOTS, 0] = g[:BG]
                made[q % SLOTS, 1] = g[BG:]
                for late in (4, 3, 2, 1):
                    stage(q, late)
                begin_when(to_hbm(q, 0))

            by = pl.BlockSpec((1, T, BC), lambda m, n: (m, 0, n))
            pltpu.emit_pipeline(body, grid=(2, GT), in_specs=[by], out_specs=[])(DG.at[layer])

            def drain(n, _):
                for late in (4, 3, 2, 1):
                    stage(steps + n, late)
                return 0

            lax.fori_loop(0, 4, drain, 0)

        five, two = pltpu.SemaphoreType.DMA((SLOTS,)), pltpu.SemaphoreType.DMA((2, 2))
        pl.run_scoped(
            scoped, pltpu.VMEM((2 * BG, T), BF16), pltpu.VMEM((SLOTS, 2, BG, BC), BF16), pltpu.VMEM((2, 1 + p, BG, BC), BF16), five, five, two)

    norm()
    on_y(Gate(0, 0))
    on_y(Gate(0, 1))
    on_c(Gate(0, 0))
    whole(Gate(0, 0))
    begin(gate_loads(0, 0))
    hooks = {2 * u: lambda u=u: (on_y(Gate(0, u + 2)), on_c(Gate(0, u + 1))) for u in range(NU - 2)}
    hooks |= {
        8: lambda: (on_y(Down(0, 0)), on_c(Gate(0, 5))),
        9: lambda: on_y(Down(0, 1)),
        10: lambda: on_c(Down(0, 0)),
        11: lambda: on_y(Down(0, 2)),
    }
    gate_up(0, hooks)
    on_c(Down(0, 1))
    on_y(Down(0, 3))
    whole(Down(0, 0))
    begin(down_loads(0, 0))
    on_c(Down(0, 2))
    whole(Down(0, 1))
    begin(down_loads(0, 1))
    whole(Down(0, 2))
    begin(down_loads(0, 2))
    on_c(Down(0, 3))
    on_y(Gate(1, 0))
    whole(Down(0, 3))
    begin(down_loads(0, 3))
    end(all_down_loads(0))
    down()
    hooks = {
        0: lambda: on_c(Gate(1, 2)),
        1: lambda: on_y(Gate(1, 4)),
        2: lambda: on_c(Gate(1, 3)),
        3: lambda: on_y(Gate(1, 5)),
        4: lambda: on_c(Gate(1, 4)),
        5: lambda: on_y(Down(1, 0)),
        6: lambda: on_c(Gate(1, 5)),
        7: lambda: (on_y(Down(1, 1)), on_c(Down(1, 0))),
        9: lambda: (on_y(Down(1, 2)), on_c(Down(1, 1))),
        11: lambda: (on_y(Down(1, 3)), on_c(Down(1, 2))),
    }
    gate_up(1, hooks)
    pltpu.make_async_copy(dy, acts.at[1], by_sem).wait()

    def backward(i, _):
        layer = 1 - i
        grad_d(layer, 0)
        end(all_down_loads(layer))
        by_hidden(layer)
        pl.when(i == 0)(lambda: begin(all_down_loads(0)))
        grad_gu(layer, 0)
        pl.when(i == 0)(by_input)
        return 0

    lax.fori_loop(0, L, backward, 0)

    tot_g[...] = jnp.zeros_like(tot_g)
    tot_d[...] = jnp.zeros_like(tot_d)

    def rest(i, _):
        grad_d(1 - i, 1)
        grad_gu(1 - i, 1)
        return 0

    lax.fori_loop(0, L, rest, 0)
    mine = tot_d[:, pl.ds(0, 128)]
    for n in range(1, D // 128):
        mine = mine + tot_d[:, pl.ds(n * 128, 128)]
    for n in range(BC // 128):
        mine = mine + tot_g[:, pl.ds(n * 128, 128)]
    sq_all[d] = mine
    exchange = [remote(sq_all.at[d], sq_all.at[d], sq_send.at[n], sq_recv.at[n], to) for n, to in enumerate((to_c, to_x, to_xc))]
    begin(exchange)
    for c in exchange:
        c.wait_recv()
    sq[...] = ((sq_all[0] + sq_all[1]) + sq_all[2]) + sq_all[3]
    for c in exchange:
        c.wait_send()

    for unit in every:
        for hop in range(4):
            for c in unit.copies(hop):
                c.wait_send()

    def sent(layer, _):
        for j in range(DT):
            for c in (d_core(layer, 0, j), d_core(layer, 1, j), d_x(layer, j)):
                c.wait_send()
        for m in range(2):
            for j in range(GT):
                g_core(2 * layer + m, 0, j).wait_send()
                g_core(2 * layer + m, 1, j).wait_send()
                g_x(2 * layer + m, j).wait_send()
        return 0

    lax.fori_loop(0, L, sent, 0)


def fused(x, dy, wg, wu, wd):
    def hbm(*shape, dtype=BF16):
        return jax.ShapeDtypeStruct(shape, dtype)

    outs = [
        hbm(L, BG, FF), hbm(L, BG, FF), hbm(L, BD, D), hbm(8, 128, dtype=F32),
        hbm(L, 2, D, FF), hbm(L, FF, D), hbm(L, D, T), hbm(T, D), hbm(L, T, FF), hbm(L, 2, T, FF, dtype=F32), hbm(L, 2, T, FF),
        hbm(4, 3, BG, FF), hbm(4, 3, BG, FF), hbm(2, 3, BD, D), hbm(2, 3, BD, D),
    ]
    specs = [ANY] * len(outs)
    specs[3] = pl.BlockSpec(memory_space=pltpu.VMEM)
    dma = pltpu.SemaphoreType.DMA
    return pl.pallas_call(
        mega,
        out_shape=outs,
        in_specs=[ANY] * 5,
        out_specs=specs,
        scratch_shapes=[
            pltpu.VMEM((2, D, FF), BF16), pltpu.VMEM((FF, D), BF16), pltpu.VMEM((2, T, D), BF16),
            pltpu.VMEM((8, FU), F32), pltpu.VMEM((8, D), F32), pltpu.VMEM((4, 8, 128), F32),
            dma((L, NU, 2, 4)), dma((L, NU, 2, 4)), dma((L, ND, 4)), dma((L, ND, 4)), dma((4, 2, 6)), dma((4, 2, 6)), dma((4, 6)), dma((4, 6)),
            dma((L, 2, 3)), dma((L, 2, 3)), dma((L, 3)), dma((L, 3)), dma((3,)), dma((3,)), dma((2, 4)), dma((4, ND)), dma,
        ],
        compiler_params=pltpu.CompilerParams(collective_id=0, has_side_effects=True, vmem_limit_bytes=67043328),
        name="step",
    )(x, dy, wg, wu, wd)[:4]


def adamw(w, m, v, g):
    m = 0.9 * m + 0.1 * g
    v = 0.95 * v + 0.05 * g * g
    step = m * lax.rsqrt(v + 1e-8) + 0.1 * w
    return (w - 0.02 * step).astype(BF16), m, v


def update(sq_ref, *refs):
    count = 4 * L * 2 * BG * FF + 4 * L * BD * D
    squares = jnp.sum(jnp.sum(sq_ref[...], axis=0, keepdims=True), axis=1, keepdims=True)
    factor = jnp.minimum(1.0, 0.5 * lax.rsqrt(squares / count + 1e-30))
    for n in range(3):
        w, m, v, g = (refs[4 * n + k] for k in range(4))
        new = adamw(w[...].astype(F32), m[...], v[...], g[...].astype(F32) * factor[None])
        for k in range(3):
            refs[12 + 3 * k + n][...] = new[k]


def updated(sq, weights, m, v, gradients):
    parts = 6
    tiles = [pl.BlockSpec((1, w.shape[1] // parts, w.shape[2]), lambda i, j: (i, j, 0)) for w in weights]
    arrays = [a for four in zip(weights, m, v, gradients, strict=True) for a in four]
    like = lambda dtype: [jax.ShapeDtypeStruct(w.shape, dtype) for w in weights]
    return pl.pallas_call(
        update,
        grid=(L, parts),
        in_specs=[pl.BlockSpec((8, 128), lambda i, j: (0, 0))] + [t for t in tiles for _ in range(4)],
        out_specs=tiles * 3,
        out_shape=like(BF16) + like(F32) + like(F32),
        compiler_params=pltpu.CompilerParams(vmem_limit_bytes=60 * 2**20),
        name="adamw",
    )(sq, *arrays)


def solution(mesh):
    def step(x, dy, *arrays):
        weights, m, v = (arrays[i : i + 3] for i in (0, 3, 6))
        *gradients, sq = fused(x[0], dy[0], *weights)
        return tuple(updated(sq, weights, m, v, gradients))

    states, cut = P(("rep", "dp"), None, None), P(None, "dp", None)
    return jax.shard_map(
        step,
        mesh=mesh,
        in_specs=(states, states) + (cut,) * 9,
        out_specs=(P("rep", "dp", None),) * 9,
        check_vma=False,
    )
```

```python
import jax
import jax.numpy as jnp
from jax import lax
from jax.experimental import pallas as pl
from jax.experimental.pallas import tpu as pltpu
from jax.sharding import PartitionSpec as P

MESH = pl.DeviceIdType.MESH
T, D, FF, L = 2048, 1152, 4608, 2
BG, BD = D // 4, FF // 4
FU = 768
NU = FF // FU
ND = 4
F32, BF16 = jnp.float32, jnp.bfloat16
ANY = pl.BlockSpec(memory_space=pl.ANY)


def nn(a, b):
    return lax.dot_general(a, b, (((1,), (0,)), ((), ())), preferred_element_type=F32)


def nt(a, b):
    return lax.dot_general(a, b, (((1,), (1,)), ((), ())), preferred_element_type=F32)


def tn(a, b):
    return lax.dot_general(a, b, (((0,), (0,)), ((), ())), preferred_element_type=F32)


def mega(x, dy, wg, wu, wd, *refs):
    (gg, gu, gd, sq, GU, WD, AT, H1, HID, PRE, DG, SG, RG, SD, RD) = refs[:15]
    (wgu, wdv, acts, tot_g, tot_d, sq_all) = refs[15:21]
    (gs, gr, ds_, dr, gcs, gcr, gxs, gxr, dcs, dcr, dxs, dxr, sq_send, sq_recv, load_sem, wd_sem, by_sem) = refs[21:]
    a_all = acts.at[0]
    r, d = lax.axis_index("rep"), lax.axis_index("dp")
    xx, cc = d // 2, d % 2
    dc, dx_, dxc = 2 * xx + 1 - cc, 2 * (1 - xx) + cc, 2 * (1 - xx) + 1 - cc
    to_c, to_x, to_xc, to_y = (r, dc), (r, dx_), (r, dxc), (1 - r, d)

    barrier = pltpu.get_barrier_semaphore()
    for to in (to_c, to_x, to_xc, to_y):
        pl.semaphore_signal(barrier, inc=1, device_id=to, device_id_type=MESH)
    pl.semaphore_wait(barrier, 4)

    def remote(src, dst, s, q, to):
        return pltpu.make_async_remote_copy(src_ref=src, dst_ref=dst, send_sem=s, recv_sem=q, device_id=to, device_id_type=MESH)

    def piece(arg, full, layer, block, r0, rows, cols, s, q, hop):
        half = rows // 2
        if hop == 0:
            mine = r0 + r * half
            return remote(arg.at[layer, pl.ds(mine, half), cols], full.at[pl.ds(d * block + mine, half), cols], s, q, to_x)
        if hop == 1:
            at = full.at[pl.ds(dx_ * block + r0 + r * half, half), cols]
            return remote(at, at, s, q, to_y)
        if hop == 2:
            return remote(arg.at[layer, pl.ds(r0, rows), cols], full.at[pl.ds(d * block + r0, rows), cols], s, q, to_c)
        at = full.at[pl.ds(dx_ * block + r0, rows), cols]
        return remote(at, at, s, q, to_c)

    def columns(u):
        return pl.ds(u * FU if isinstance(u, int) else pl.multiple_of(u * FU, FU), FU)

    class Gate:
        def __init__(self, layer, u):
            self.layer, self.u = layer, u

        def copies(self, hop):
            layer, u = self.layer, self.u
            return [piece(arg, GU.at[layer, m], layer, BG, 0, BG, columns(u), gs.at[layer, u, m, hop], gr.at[layer, u, m, hop], hop)
                    for m, arg in enumerate((wg, wu))]

    class Down:
        def __init__(self, layer, u):
            self.layer, self.u = layer, u

        def copies(self, hop):
            layer, u = self.layer, self.u
            return [piece(wd, WD.at[layer], layer, BD, u * (BD // ND), BD // ND, pl.ds(0, D), ds_.at[layer, u, hop], dr.at[layer, u, hop], hop)]

    def start(unit, hop):
        for c in unit.copies(hop):
            c.start()

    def arrive(unit, hop):
        for c in unit.copies(hop):
            c.wait_recv()

    def on_y(unit):
        arrive(unit, 0)
        start(unit, 1)

    def on_c(unit):
        arrive(unit, 1)
        start(unit, 3)

    def whole(unit):
        arrive(unit, 2)
        arrive(unit, 3)

    every = [unit(layer, u) for layer in range(L) for unit, n in ((Gate, NU), (Down, ND)) for u in range(n)]
    for unit in every:
        start(unit, 0)
    for unit in every:
        start(unit, 2)
    pltpu.make_async_copy(dy, acts.at[1], by_sem).start()

    def gate_loads(layer, u):
        out = []
        for m, arg in enumerate((wg, wu)):
            for i, b in enumerate((d, dc, dx_, dxc)):
                rows = pl.ds(b * BG, BG)
                src = GU.at[layer, m, rows, columns(u)] if i else arg.at[layer, :, columns(u)]
                out.append(pltpu.make_async_copy(src, wgu.at[m, rows, columns(u)], load_sem.at[m, i]))
        return out

    def down_loads(layer, u):
        out = []
        for i, b in enumerate((d, dc, dx_, dxc)):
            part = pl.ds(u * (BD // ND), BD // ND)
            rows = pl.ds(b * BD + u * (BD // ND), BD // ND)
            out.append(pltpu.make_async_copy(WD.at[layer, rows, :] if i else wd.at[layer, part, :], wdv.at[rows, :], wd_sem.at[i, u]))
        return out

    def all_down_loads(layer):
        return [c for u in range(ND) for c in down_loads(layer, u)]

    def begin(copies):
        for c in copies:
            c.start()

    def end(copies):
        for c in copies:
            c.wait()

    def begin_when(cases):
        for when, c in cases:
            if when is True:
                c.start()
            else:
                pl.when(when)(c.start)

    def end_when(cases):
        for when, c in cases:
            if when is True:
                c.wait()
            else:
                pl.when(when)(c.wait)

    def norm_of(h):
        wide = h.astype(F32)
        scale = lax.rsqrt(jnp.mean(wide * wide, -1, keepdims=True) + 1e-6)
        return wide * scale

    def rows_of(i, b):
        return pl.ds(pl.multiple_of(i * b, b), b)

    def at_steps(step, hooks):
        for when, what in hooks.items():

            @pl.when(step == when)
            def _(what=what):
                what()

    def norm():
        b = 512

        def body(x_ref, at_ref):
            a = norm_of(x_ref[...])
            a_all[rows_of(pl.program_id(0), b), :] = a.astype(BF16)
            at_ref[...] = a.T.astype(BF16)

        pltpu.emit_pipeline(
            body, grid=(T // b,), in_specs=[pl.BlockSpec((b, D), lambda i: (i, 0))], out_specs=[pl.BlockSpec((D, b), lambda i: (0, i))],
        )(x, AT.at[0])

    def gate_up(layer, hooks):
        b = 1024

        def body(gate_ref, up_ref, hid_ref):
            u, t = pl.program_id(0), pl.program_id(1)
            pl.when(t == 0)(lambda: end(gate_loads(layer, u)))
            at_steps(2 * u + t, hooks)
            a = a_all[rows_of(t, b), :]

            @pl.when((t == 1) & (u + 1 < NU))
            def _():
                whole(Gate(layer, u + 1))
                begin(gate_loads(layer, u + 1))

            gate = nn(a, wgu[0, :, columns(u)])
            gate_ref[...] = gate
            up = nn(a, wgu[1, :, columns(u)])
            up_ref[...] = up
            hid_ref[...] = (gate * jax.nn.sigmoid(gate) * up).astype(BF16)

        tile = pl.BlockSpec((b, FU), lambda u, t: (t, u))
        pltpu.emit_pipeline(body, grid=(NU, T // b), in_specs=[], out_specs=[tile] * 3)(PRE.at[layer, 0], PRE.at[layer, 1], HID.at[layer])

    def down():
        b = 256

        def body(x_ref, hid_ref, h_ref, at_ref):
            i = pl.program_id(0)
            at_steps(i, {
                2: lambda: on_y(Gate(1, 1)),
                3: lambda: on_c(Gate(1, 0)),
                5: lambda: (on_y(Gate(1, 2)), on_c(Gate(1, 1))),
                7: lambda: (on_y(Gate(1, 3)), whole(Gate(1, 0)), begin(gate_loads(1, 0))),
            })
            h = x_ref[...] + nn(hid_ref[...], wdv[...]).astype(BF16)
            h_ref[...] = h
            a = norm_of(h)
            a_all[rows_of(i, b), :] = a.astype(BF16)
            at_ref[...] = a.T.astype(BF16)

        row = pl.BlockSpec((b, D), lambda i: (i, 0))
        pltpu.emit_pipeline(
            body, grid=(T // b,), in_specs=[row, pl.BlockSpec((b, FF), lambda i: (i, 0))],
            out_specs=[row, pl.BlockSpec((D, b), lambda i: (0, i))],
        )(x, HID.at[0], H1, AT.at[1])

    def by_hidden(layer):
        b, n = 512, 1152

        def body(gate_ref, up_ref, bg_ref, bu_ref):
            i, j = pl.program_id(0), pl.program_id(1)
            by_hid = nt(acts[layer, rows_of(i, b), :], wdv[rows_of(j, n), :]).astype(BF16).astype(F32)
            gate, up = gate_ref[...], up_ref[...]
            s = jax.nn.sigmoid(gate)
            silu = gate * s
            bu_ref[...] = (by_hid * silu).astype(BF16)
            bg_ref[...] = (by_hid * up * (s + silu * (1 - s))).astype(BF16)

        deep = pl.BlockSpec((b, n), lambda i, j: (i, j), pipeline_mode=pl.Buffered(3))
        tile = pl.BlockSpec((b, n), lambda i, j: (i, j))
        pltpu.emit_pipeline(body, grid=(T // b, FF // n), in_specs=[deep, deep], out_specs=[tile, tile])(
            PRE.at[layer, 0], PRE.at[layer, 1], DG.at[layer, 0], DG.at[layer, 1])

    def by_input():
        b = 256

        def body(bg_ref, bu_ref, h_ref):
            rows = rows_of(pl.program_id(0), b)
            by_a = nt(bg_ref[...], wgu[0]).astype(BF16).astype(F32) + nt(bu_ref[...], wgu[1]).astype(BF16).astype(F32)
            by_a = by_a.astype(BF16).astype(F32)
            wide = h_ref[...].astype(F32)
            scale = lax.rsqrt(jnp.mean(wide * wide, -1, keepdims=True) + 1e-6)
            along = jnp.mean(by_a * wide, -1, keepdims=True)
            by_h = by_a * scale - wide * (scale * scale * scale * along)
            acts[0, rows, :] = acts[1, rows, :] + by_h.astype(BF16)

        row, wide_row = pl.BlockSpec((b, D), lambda i: (i, 0)), pl.BlockSpec((b, FF), lambda i: (i, 0))
        pltpu.emit_pipeline(body, grid=(T // b,), in_specs=[wide_row, wide_row, row], out_specs=[])(DG.at[1, 0], DG.at[1, 1], H1)

    def block_of(k):
        return 2 * ((1 - xx) * (1 - k // 2) + xx * (k // 2)) + (1 - cc) * (1 - k % 2) + cc * (k % 2)

    BT, BC = 384, 768
    DT, GT, SLOTS = BD // BT, FF // BC, 5

    def d_rows(j):
        return pl.ds(pl.multiple_of(j * BT, BT), BT)

    def d_core(layer, p, j):
        at = (layer, 2 * p, d_rows(j), slice(None))
        return remote(SD.at[at], RD.at[at], dcs.at[layer, p, j], dcr.at[layer, p, j], to_c)

    def d_x(layer, j):
        at = (layer, 1, d_rows(j), slice(None))
        return remote(SD.at[at], RD.at[at], dxs.at[layer, j], dxr.at[layer, j], to_x)

    def g_cols(j):
        return pl.ds(pl.multiple_of(j * BC, BC), BC)

    def g_core(i, p, j):
        at = (i, 2 * p, slice(None), g_cols(j))
        return remote(SG.at[at], RG.at[at], gcs.at[i, p, j], gcr.at[i, p, j], to_c)

    def g_x(i, j):
        at = (i, 1, slice(None), g_cols(j))
        return remote(SG.at[at], RG.at[at], gxs.at[i, j], gxr.at[i, j], to_x)

    def square(total, g, cols):
        g = g.astype(F32)
        total[...] += jnp.sum((g * g).reshape(g.shape[0] // 8, 8, cols), axis=0)

    def grad_d(layer, p):
        def scoped(made, came, made_sem, came_sem):
            def to_hbm(n):
                def copy(dst):
                    return pltpu.make_async_copy(made.at[n % 2], dst, made_sem.at[n % 2])

                stage = copy(SD.at[layer, 2 * p + n // DT * (1 - p), d_rows(n % DT), :])
                return [(n < DT, stage), (n >= DT, copy(gd.at[layer, d_rows(n % DT), :]))] if p else [(True, stage)]

            def from_hbm(j, k):
                src = RD.at[layer, 1 if k else 2 * p, d_rows(j), :]
                return pltpu.make_async_copy(src, came.at[j % 2, k], came_sem.at[j % 2, k])

            def fetch(j):
                d_core(layer, p, j).wait_recv()
                from_hbm(j, 0).start()
                if p:
                    d_x(layer, j).wait_recv()
                    from_hbm(j, 1).start()

            def send(n):
                end_when(to_hbm(n))
                pl.when(n < DT)(lambda: d_core(layer, p, n % DT).start())
                if p == 0:
                    pl.when(n >= DT)(lambda: d_x(layer, n % DT).start())

            def body(hid_ref):
                n = pl.program_id(0)
                if p == 0:
                    pl.when((layer == 1) & (n == 3))(lambda: on_c(Down(1, 3)))

                    @pl.when((layer == 1) & (n == 5))
                    def _():
                        for u in range(ND):
                            whole(Down(1, u))
                        begin(all_down_loads(1))

                made[n % 2] = tn(hid_ref[...], acts[layer]).astype(BF16)

                @pl.when(n >= DT)
                def _():
                    j = n % DT
                    from_hbm(j, 0).wait()
                    g = made[n % 2].astype(F32) + came[j % 2, 0].astype(F32)
                    if p:
                        from_hbm(j, 1).wait()
                        g = g + came[j % 2, 1].astype(F32)
                    g = g.astype(BF16)
                    made[n % 2] = g
                    if p:
                        square(tot_d, g, D)

                begin_when(to_hbm(n))
                pl.when(n > 0)(lambda: send(n - 1))
                pl.when((n >= DT - 1) & (n < 2 * DT - 1))(lambda: fetch(n - (DT - 1)))

            hid = pl.BlockSpec((T, BT), lambda n: (0, block_of(2 * p + n // DT) * DT + n % DT))
            pltpu.emit_pipeline(body, grid=(2 * DT,), in_specs=[hid], out_specs=[])(HID.at[layer])
            send(2 * DT - 1)

        dma = pltpu.SemaphoreType.DMA
        pl.run_scoped(scoped, pltpu.VMEM((2, BT, D), BF16), pltpu.VMEM((2, 1 + p, BT, D), BF16), dma((2,)), dma((2, 2)))

    def grad_gu(layer, p):
        steps = 2 * GT

        def scoped(lhs, made, came, made_sem, own_sem, came_sem):
            rows = [
                pltpu.make_async_copy(AT.at[layer, pl.ds(block_of(2 * p + h) * BG, BG), :], lhs.at[pl.ds(h * BG, BG), :], load_sem.at[0, h])
                for h in range(2)
            ]

            def to_hbm(q, h):
                m, cols = q // GT, g_cols(q % GT)

                def copy(dst):
                    return pltpu.make_async_copy(made.at[q % SLOTS, h], dst, (made_sem, own_sem)[h].at[q % SLOTS])

                if p and h:
                    return [(m == 0, copy(gg.at[layer, :, cols])), (m == 1, copy(gu.at[layer, :, cols]))]
                return [(True, copy(SG.at[2 * layer + m, 2 * p + h, :, cols]))]

            def from_hbm(q, k):
                src = RG.at[2 * layer + q // GT, 1 if k else 2 * p, :, g_cols(q % GT)]
                return pltpu.make_async_copy(src, came.at[q % 2, k], came_sem.at[q % 2, k])

            def stage_1(q):
                end_when(to_hbm(q, 0))
                g_core(2 * layer + q // GT, p, q % GT).start()

            def stage_2(q):
                i, j = 2 * layer + q // GT, q % GT
                g_core(i, p, j).wait_recv()
                from_hbm(q, 0).start()
                if p:
                    g_x(i, j).wait_recv()
                    from_hbm(q, 1).start()

            def stage_3(q):
                from_hbm(q, 0).wait()
                g = made[q % SLOTS, 1].astype(F32) + came[q % 2, 0].astype(F32)
                if p:
                    from_hbm(q, 1).wait()
                    g = g + came[q % 2, 1].astype(F32)
                g = g.astype(BF16)
                made[q % SLOTS, 1] = g
                if p:
                    square(tot_g, g, BC)
                begin_when(to_hbm(q, 1))

            def stage_4(q):
                end_when(to_hbm(q, 1))
                if p == 0:
                    g_x(2 * layer + q // GT, q % GT).start()

            def stage(q, late):
                what = (stage_1, stage_2, stage_3, stage_4)[late - 1]
                pl.when((q >= late) & (q < steps + late))(lambda: what(q - late))

            begin(rows)

            def body(by_ref):
                q = GT * pl.program_id(0) + pl.program_id(1)
                pl.when(q == 0)(lambda: end(rows))
                g = nn(lhs[...], by_ref[0]).astype(BF16)
                made[q % SLOTS, 0] = g[:BG]
                made[q % SLOTS, 1] = g[BG:]
                for late in (4, 3, 2, 1):
                    stage(q, late)
                begin_when(to_hbm(q, 0))

            by = pl.BlockSpec((1, T, BC), lambda m, n: (m, 0, n))
            pltpu.emit_pipeline(body, grid=(2, GT), in_specs=[by], out_specs=[])(DG.at[layer])

            def drain(n, _):
                for late in (4, 3, 2, 1):
                    stage(steps + n, late)
                return 0

            lax.fori_loop(0, 4, drain, 0)

        five, two = pltpu.SemaphoreType.DMA((SLOTS,)), pltpu.SemaphoreType.DMA((2, 2))
        pl.run_scoped(
            scoped, pltpu.VMEM((2 * BG, T), BF16), pltpu.VMEM((SLOTS, 2, BG, BC), BF16), pltpu.VMEM((2, 1 + p, BG, BC), BF16), five, five, two)

    norm()
    on_y(Gate(0, 0))
    on_y(Gate(0, 1))
    on_c(Gate(0, 0))
    whole(Gate(0, 0))
    begin(gate_loads(0, 0))
    hooks = {2 * u: lambda u=u: (on_y(Gate(0, u + 2)), on_c(Gate(0, u + 1))) for u in range(NU - 2)}
    hooks |= {
        8: lambda: (on_y(Down(0, 0)), on_c(Gate(0, 5))),
        9: lambda: on_y(Down(0, 1)),
        10: lambda: on_c(Down(0, 0)),
        11: lambda: on_y(Down(0, 2)),
    }
    gate_up(0, hooks)
    on_c(Down(0, 1))
    on_y(Down(0, 3))
    whole(Down(0, 0))
    begin(down_loads(0, 0))
    on_c(Down(0, 2))
    whole(Down(0, 1))
    begin(down_loads(0, 1))
    whole(Down(0, 2))
    begin(down_loads(0, 2))
    on_c(Down(0, 3))
    on_y(Gate(1, 0))
    whole(Down(0, 3))
    begin(down_loads(0, 3))
    end(all_down_loads(0))
    down()
    hooks = {
        0: lambda: on_c(Gate(1, 2)),
        1: lambda: on_y(Gate(1, 4)),
        2: lambda: on_c(Gate(1, 3)),
        3: lambda: on_y(Gate(1, 5)),
        4: lambda: on_c(Gate(1, 4)),
        5: lambda: on_y(Down(1, 0)),
        6: lambda: on_c(Gate(1, 5)),
        7: lambda: (on_y(Down(1, 1)), on_c(Down(1, 0))),
        9: lambda: (on_y(Down(1, 2)), on_c(Down(1, 1))),
        11: lambda: (on_y(Down(1, 3)), on_c(Down(1, 2))),
    }
    gate_up(1, hooks)
    pltpu.make_async_copy(dy, acts.at[1], by_sem).wait()

    def backward(i, _):
        layer = 1 - i
        grad_d(layer, 0)
        end(all_down_loads(layer))
        by_hidden(layer)
        pl.when(i == 0)(lambda: begin(all_down_loads(0)))
        grad_gu(layer, 0)
        pl.when(i == 0)(by_input)
        return 0

    lax.fori_loop(0, L, backward, 0)

    tot_g[...] = jnp.zeros_like(tot_g)
    tot_d[...] = jnp.zeros_like(tot_d)

    def rest(i, _):
        grad_d(1 - i, 1)
        grad_gu(1 - i, 1)
        return 0

    lax.fori_loop(0, L, rest, 0)
    mine = tot_d[:, pl.ds(0, 128)]
    for n in range(1, D // 128):
        mine = mine + tot_d[:, pl.ds(n * 128, 128)]
    for n in range(BC // 128):
        mine = mine + tot_g[:, pl.ds(n * 128, 128)]
    sq_all[d] = mine
    exchange = [remote(sq_all.at[d], sq_all.at[d], sq_send.at[n], sq_recv.at[n], to) for n, to in enumerate((to_c, to_x, to_xc))]
    begin(exchange)
    for c in exchange:
        c.wait_recv()
    sq[...] = ((sq_all[0] + sq_all[1]) + sq_all[2]) + sq_all[3]
    for c in exchange:
        c.wait_send()

    for unit in every:
        for hop in range(4):
            for c in unit.copies(hop):
                c.wait_send()

    def sent(layer, _):
        for j in range(DT):
            for c in (d_core(layer, 0, j), d_core(layer, 1, j), d_x(layer, j)):
                c.wait_send()
        for m in range(2):
            for j in range(GT):
                g_core(2 * layer + m, 0, j).wait_send()
                g_core(2 * layer + m, 1, j).wait_send()
                g_x(2 * layer + m, j).wait_send()
        return 0

    lax.fori_loop(0, L, sent, 0)


def fused(x, dy, wg, wu, wd):
    def hbm(*shape, dtype=BF16):
        return jax.ShapeDtypeStruct(shape, dtype)

    outs = [
        hbm(L, BG, FF), hbm(L, BG, FF), hbm(L, BD, D), hbm(8, 128, dtype=F32),
        hbm(L, 2, D, FF), hbm(L, FF, D), hbm(L, D, T), hbm(T, D), hbm(L, T, FF), hbm(L, 2, T, FF, dtype=F32), hbm(L, 2, T, FF),
        hbm(4, 3, BG, FF), hbm(4, 3, BG, FF), hbm(2, 3, BD, D), hbm(2, 3, BD, D),
    ]
    specs = [ANY] * len(outs)
    specs[3] = pl.BlockSpec(memory_space=pltpu.VMEM)
    dma = pltpu.SemaphoreType.DMA
    return pl.pallas_call(
        mega,
        out_shape=outs,
        in_specs=[ANY] * 5,
        out_specs=specs,
        scratch_shapes=[
            pltpu.VMEM((2, D, FF), BF16), pltpu.VMEM((FF, D), BF16), pltpu.VMEM((2, T, D), BF16),
            pltpu.VMEM((8, FU), F32), pltpu.VMEM((8, D), F32), pltpu.VMEM((4, 8, 128), F32),
            dma((L, NU, 2, 4)), dma((L, NU, 2, 4)), dma((L, ND, 4)), dma((L, ND, 4)), dma((4, 2, 6)), dma((4, 2, 6)), dma((4, 6)), dma((4, 6)),
            dma((L, 2, 3)), dma((L, 2, 3)), dma((L, 3)), dma((L, 3)), dma((3,)), dma((3,)), dma((2, 4)), dma((4, ND)), dma,
        ],
        compiler_params=pltpu.CompilerParams(collective_id=0, has_side_effects=True, vmem_limit_bytes=67043328),
        name="step",
    )(x, dy, wg, wu, wd)[:4]


def adamw(w, m, v, g):
    m = 0.9 * m + 0.1 * g
    v = 0.95 * v + 0.05 * g * g
    step = m * lax.rsqrt(v + 1e-8) + 0.1 * w
    return (w - 0.02 * step).astype(BF16), m, v


def update(sq_ref, *refs):
    count = 4 * L * 2 * BG * FF + 4 * L * BD * D
    squares = jnp.sum(jnp.sum(sq_ref[...], axis=0, keepdims=True), axis=1, keepdims=True)
    factor = jnp.minimum(1.0, 0.5 * lax.rsqrt(squares / count + 1e-30))
    for n in range(3):
        w, m, v, g = (refs[4 * n + k] for k in range(4))
        new = adamw(w[...].astype(F32), m[...], v[...], g[...].astype(F32) * factor[None])
        for k in range(3):
            refs[12 + 3 * k + n][...] = new[k]


def updated(sq, weights, m, v, gradients):
    parts = 9
    tiles = [pl.BlockSpec((1, w.shape[1] // parts, w.shape[2]), lambda i, j: (i, j, 0)) for w in weights]
    arrays = [a for four in zip(weights, m, v, gradients, strict=True) for a in four]
    like = lambda dtype: [jax.ShapeDtypeStruct(w.shape, dtype) for w in weights]
    return pl.pallas_call(
        update,
        grid=(L, parts),
        in_specs=[pl.BlockSpec((8, 128), lambda i, j: (0, 0))] + [t for t in tiles for _ in range(4)],
        out_specs=tiles * 3,
        out_shape=like(BF16) + like(F32) + like(F32),
        compiler_params=pltpu.CompilerParams(vmem_limit_bytes=60 * 2**20),
        name="adamw",
    )(sq, *arrays)


def solution(mesh):
    def step(x, dy, *arrays):
        weights, m, v = (arrays[i : i + 3] for i in (0, 3, 6))
        *gradients, sq = fused(x[0], dy[0], *weights)
        return tuple(updated(sq, weights, m, v, gradients))

    states, cut = P(("rep", "dp"), None, None), P(None, "dp", None)
    return jax.shard_map(
        step,
        mesh=mesh,
        in_specs=(states, states) + (cut,) * 9,
        out_specs=(P("rep", "dp", None),) * 9,
        check_vma=False,
    )
```
